16 devices in a mesh: dp: 2 (over y, z), cp: 8 (over x, core).
Axes of the slice: x: 4, y: 2, z: 1, core: 2. Of those that a mesh axis runs over, the one named last changes fastest.
The devices are a block of a 4x4x8 slice.
Arguments:
- x_tok: bfloat16 [128, 3584], P(('dp', 'cp')), parts along dimension 0
- prompt_lens: int32 [128], P('dp'), parts along dimension 0
- k_cache: bfloat16 [128, 512, 4, 128], P('dp', 'cp'), parts along dimension 0
- v_cache: bfloat16 [128, 512, 4, 128], P('dp', 'cp'), parts along dimension 0
- norm_gain: bfloat16 [3584], replicated
- w_q: bfloat16 [3584, 3584], replicated
- b_q: bfloat16 [3584], replicated
- w_k: bfloat16 [3584, 512], replicated
- b_k: bfloat16 [512], replicated
- w_v: bfloat16 [3584, 512], replicated
- b_v: bfloat16 [512], replicated
- w_o: bfloat16 [3584, 3584], replicated
Outputs:
- output 1: bfloat16 [128, 3584], P(('dp', 'cp')), parts along dimension 0
- output 2: bfloat16 [128, 512, 4, 128], P(('dp', 'cp')), parts along dimension 0
- output 3: bfloat16 [128, 512, 4, 128], P(('dp', 'cp')), parts along dimension 0
There are 2 independent parts. The reference program is written for one: setup_inputs(seed, part) draws one part's arguments, and reference() takes and returns one part's arrays. A program takes and returns all parts, laid end to end along the dimension named above; an argument that names none is the same for every part.
All inputs are finite; a program needn't handle non-finite values.
Results may differ from the reference program's by a relative error of at most 0.00931332.
Values are sent between devices in bfloat16 or wider.
A program may use at most 768 MiB of HBM per device.

```python
import math
import jax
import jax.numpy as jnp
from jax import lax

D = 3584
HEADS = 28
KV_HEADS = 4
HEAD = 128
BATCH = 64
SEQ = 512

GROUP = HEADS // KV_HEADS
HALF = HEAD // 2
RMS_EPS = 1e-6
ROPE_THETA = 1000000.0
SCORE_SCALE = HEAD ** -0.5


def normal_draw(draw_key, shape, scale):
    return (jax.random.normal(draw_key, shape, jnp.float32) * scale).astype(jnp.bfloat16)


def setup_inputs(seed: int = 0, part: int = 0) -> dict:
    base_key = jax.random.key(seed)
    part_keys = jax.random.split(jax.random.fold_in(base_key, part), 5)
    weight_keys = jax.random.split(base_key, 8)
    gain = math.sqrt(SEQ) / 4.0
    low_len = SEQ // 16
    prompt_lens = jax.random.randint(part_keys[1], (BATCH,), low_len, SEQ, jnp.int32)
    order = jax.random.permutation(part_keys[2], BATCH)
    prompt_lens = prompt_lens.at[order[0]].set(SEQ - 1).at[order[1]].set(low_len)
    norm_gain = (1.0 + 0.3 * jax.random.normal(weight_keys[0], (D,), jnp.float32)).astype(jnp.bfloat16)
    return {
        'x_tok': normal_draw(part_keys[0], (BATCH, D), 1.0),
        'prompt_lens': prompt_lens,
        'k_cache': normal_draw(part_keys[3], (BATCH, SEQ, KV_HEADS, HEAD), 1.0),
        'v_cache': normal_draw(part_keys[4], (BATCH, SEQ, KV_HEADS, HEAD), 1.0),
        'norm_gain': norm_gain,
        'w_q': normal_draw(weight_keys[1], (D, HEADS * HEAD), D ** -0.5),
        'b_q': normal_draw(weight_keys[2], (HEADS * HEAD,), 0.5),
        'w_k': normal_draw(weight_keys[3], (D, KV_HEADS * HEAD), D ** -0.5),
        'b_k': normal_draw(weight_keys[4], (KV_HEADS * HEAD,), 1.0),
        'w_v': normal_draw(weight_keys[5], (D, KV_HEADS * HEAD), gain * D ** -0.5),
        'b_v': normal_draw(weight_keys[6], (KV_HEADS * HEAD,), 0.5 * gain),
        'w_o': normal_draw(weight_keys[7], (HEADS * HEAD, D), gain * (HEADS * HEAD) ** -0.5),
    }


def rotary(vectors, positions):
    inv_freq = jnp.power(ROPE_THETA, -(jnp.arange(HALF).astype(jnp.float32) * 2.0 / HEAD))
    angle = positions.astype(jnp.float32)[:, None, None] * inv_freq
    cos_t = jnp.cos(angle)
    sin_t = jnp.sin(angle)
    first = vectors[..., :HALF]
    second = vectors[..., HALF:]
    return jnp.concatenate([first * cos_t - second * sin_t, second * cos_t + first * sin_t], axis=-1)


def reference(x_tok, prompt_lens, k_cache, v_cache, norm_gain, w_q, b_q, w_k, b_k, w_v, b_v, w_o):
    x_wide = x_tok.astype(jnp.float32)
    mean_sq = jnp.mean(x_wide * x_wide, axis=-1, keepdims=True)
    normed = (x_wide * lax.rsqrt(mean_sq + RMS_EPS) * norm_gain.astype(jnp.float32)).astype(jnp.bfloat16)
    query = jnp.dot(normed, w_q, preferred_element_type=jnp.float32) + b_q.astype(jnp.float32)
    query = rotary(query.reshape(BATCH, HEADS, HEAD), prompt_lens).astype(jnp.bfloat16)
    key_new = jnp.dot(normed, w_k, preferred_element_type=jnp.float32) + b_k.astype(jnp.float32)
    key_new = rotary(key_new.reshape(BATCH, KV_HEADS, HEAD), prompt_lens).astype(jnp.bfloat16)
    value_new = jnp.dot(normed, w_v, preferred_element_type=jnp.float32) + b_v.astype(jnp.float32)
    value_new = value_new.reshape(BATCH, KV_HEADS, HEAD).astype(jnp.bfloat16)
    slot_idx = jnp.arange(SEQ)

    def one_sequence(operands):
        keys_old, vals_old, query_one, key_one, value_one, length = operands
        before = (slot_idx < length)[:, None, None]
        at_new = (slot_idx == length)[:, None, None]
        keys_all = jnp.where(at_new, key_one[None], jnp.where(before, keys_old, jnp.zeros_like(keys_old)))
        vals_all = jnp.where(at_new, value_one[None], jnp.where(before, vals_old, jnp.zeros_like(vals_old)))
        scores = jnp.einsum('kgd,skd->kgs', query_one.reshape(KV_HEADS, GROUP, HEAD).astype(jnp.float32), keys_all.astype(jnp.float32)) * SCORE_SCALE
        scores = jnp.where(slot_idx <= length, scores, -1e30)
        row_max = jnp.max(scores, axis=-1, keepdims=True)
        weights = jnp.exp(scores - row_max)
        weight_sum = jnp.sum(weights, axis=-1, keepdims=True)
        mixed = jnp.einsum('kgs,skd->kgd', weights.astype(jnp.bfloat16).astype(jnp.float32), vals_all.astype(jnp.float32)) / weight_sum
        return keys_all, vals_all, mixed.reshape(HEADS * HEAD).astype(jnp.bfloat16)

    k_out, v_out, attended = lax.map(one_sequence, (k_cache, v_cache, query, key_new, value_new, prompt_lens))
    y_out = (x_wide + jnp.dot(attended, w_o, preferred_element_type=jnp.float32)).astype(jnp.bfloat16)
    return y_out, k_out, v_out
```

```python
import functools

import jax
import jax.numpy as jnp
from jax import lax
from jax.experimental import pallas as pl
from jax.experimental.pallas import tpu as pltpu
from jax.sharding import PartitionSpec as P

RMS_EPS = 1e-6
ROPE_THETA = 1000000.0
PACK = 16
NEG = -1e30


def gather_kernel(n, kv_heads, lens_hbm, x_hbm, rot_hbm, gain_hbm, wq_hbm, bq_hbm, wk_hbm, bk_hbm, wv_hbm, bv_hbm, wo_hbm, k_hbm, v_hbm,
                  kbuf, vbuf, wo_ref, att_ref,
                  lens, x_ref, rot_ref, gain_ref, bq_ref, bk_ref, bv_ref, wbuf, h_ref, qf_ref, knew_ref, vnew_ref, s_ref, p_ref, acc_ref, sum_ref,
                  small_sem, wsem, wo_sem, local_sem, send_sem, recv_sem):
    rows, d_model = x_ref.shape
    head = acc_ref.shape[-1]
    q_rows = acc_ref.shape[1]
    heads = att_ref.shape[1] // head
    group = heads // kv_heads
    tiles = k_hbm.shape[1]
    block_rows = tiles * PACK
    slots = block_rows // kv_heads
    cols = wbuf.shape[2]
    me = lax.axis_index('cp')

    smalls = [
        pltpu.make_async_copy(src, dst, small_sem.at[i])
        for i, (src, dst) in enumerate([
            (lens_hbm, lens), (x_hbm, x_ref), (rot_hbm, rot_ref), (gain_hbm, gain_ref), (bq_hbm, bq_ref), (bk_hbm, bk_ref), (bv_hbm, bv_ref)])
    ]
    for copy in smalls:
        copy.start()

    blocks = [(wk_hbm, 0), (wv_hbm, 0)] + [(wq_hbm, c) for c in range(wq_hbm.shape[1] // cols)]

    def weight_copy(t):
        src, c = blocks[t]
        return pltpu.make_async_copy(src.at[:, pl.ds(c * cols, cols)], wbuf.at[t % wbuf.shape[0]], wsem.at[t % wbuf.shape[0]])

    for t in range(wbuf.shape[0]):
        weight_copy(t).start()

    def block_of(ref, owner):
        return ref.at[pl.ds(owner * rows, rows)]

    def place_of(ref, sender):
        return ref.at[:, pl.ds(sender * tiles, tiles)]

    own_k = pltpu.make_async_copy(block_of(k_hbm, me), place_of(kbuf, me), local_sem.at[0])
    own_v = pltpu.make_async_copy(block_of(v_hbm, me), place_of(vbuf, me), local_sem.at[1])
    own_k.start()
    own_v.start()

    barrier = pltpu.get_barrier_semaphore()
    peers = [lax.rem(me + k, n) for k in range(1, n)]
    for peer in peers:
        pl.semaphore_signal(barrier, inc=1, device_id={'cp': peer}, device_id_type=pl.DeviceIdType.MESH)
    pl.semaphore_wait(barrier, n - 1)

    chip, core = me // 2, lax.rem(me, 2)
    chips = n // 2

    def device(far, other):
        return lax.rem(chip + far, chips) * 2 + (core + other) % 2

    order = [(0, 1)]
    fars = sorted(range(1, chips), key=lambda f: -min(f, chips - f))
    for far in fars:
        order += [(far, 0), (far, 1)]

    def remote(which, src, dst, to):
        return pltpu.make_async_remote_copy(
            src_ref=block_of(src, to), dst_ref=place_of(dst, me),
            send_sem=send_sem.at[which, to], recv_sem=recv_sem.at[which, me],
            device_id={'cp': to}, device_id_type=pl.DeviceIdType.MESH)

    def arrival(which, src, dst, sender):
        return pltpu.make_async_remote_copy(
            src_ref=block_of(src, sender), dst_ref=place_of(dst, sender),
            send_sem=send_sem.at[which, sender], recv_sem=recv_sem.at[which, sender],
            device_id={'cp': sender}, device_id_type=pl.DeviceIdType.MESH)

    sends = []
    for which, (src, dst) in enumerate([(k_hbm, kbuf), (v_hbm, vbuf)]):
        for far, other in order:
            copy = remote(which, src, dst, device(far, other))
            copy.start()
            sends.append(copy)

    for copy in smalls:
        copy.wait()
    x_wide = x_ref[...].astype(jnp.float32)
    mean_sq = jnp.mean(x_wide * x_wide, axis=-1, keepdims=True)
    h_ref[...] = (x_wide * lax.rsqrt(mean_sq + RMS_EPS) * gain_ref[...].astype(jnp.float32)).astype(jnp.bfloat16)
    cos_t = rot_ref[0]
    sin_t = rot_ref[1]

    def rotate(v):
        return v * cos_t + pltpu.roll(v, head // 2, 1) * sin_t

    qf_ref[...] = jnp.zeros_like(qf_ref)
    for t in range(len(blocks)):
        weight_copy(t).wait()
        out = jnp.dot(h_ref[...], wbuf[t % wbuf.shape[0]], preferred_element_type=jnp.float32)
        if t + wbuf.shape[0] < len(blocks):
            weight_copy(t + wbuf.shape[0]).start()
        c = blocks[t][1]
        bias = (bk_ref if t == 0 else bv_ref if t == 1 else bq_ref)[:, c * cols:(c + 1) * cols]
        out = out + bias.astype(jnp.float32)
        for i in range(cols // head):
            part = out[:, i * head:(i + 1) * head]
            if t == 0:
                part = rotate(part).astype(jnp.bfloat16).astype(jnp.float32)
                for r in range(PACK // kv_heads):
                    knew_ref[:, r * kv_heads + i, :] = part
            elif t == 1:
                part = part.astype(jnp.bfloat16).astype(jnp.float32)
                for r in range(PACK // kv_heads):
                    vnew_ref[:, r * kv_heads + i, :] = part
            else:
                qf_ref[:, c * (cols // head) + i, :] = rotate(part)
    wo_copy = pltpu.make_async_copy(wo_hbm, wo_ref, wo_sem)
    wo_copy.start()

    def merged(s, sender, buf, new_ref):
        pos = lens[0, me * rows + s]
        tile = buf[s, pl.ds(sender * tiles, tiles)].astype(jnp.float32)
        shape = (tiles, PACK, head)
        slot = sender * slots + lax.broadcasted_iota(jnp.int32, shape, 0) * (PACK // kv_heads) + lax.broadcasted_iota(jnp.int32, shape, 1) // kv_heads
        new = jnp.broadcast_to(new_ref[s][None], shape)
        tile = jnp.where(slot < pos, tile, jnp.where(slot == pos, new, 0.0)).astype(jnp.bfloat16)
        buf[s, pl.ds(sender * tiles, tiles)] = tile
        return tile.reshape(block_rows, head)

    def keys_step(s, sender):
        pos = lens[0, me * rows + s]
        keys = merged(s, sender, kbuf, knew_ref)
        query = qf_ref[s].astype(jnp.bfloat16)
        scores = lax.dot_general(query, keys, (((1,), (1,)), ((), ())), preferred_element_type=jnp.float32) * (head ** -0.5)
        row = lax.broadcasted_iota(jnp.int32, scores.shape, 0)
        col = lax.broadcasted_iota(jnp.int32, scores.shape, 1)
        valid = (col % kv_heads == row // group) & (sender * slots + col // kv_heads <= pos)
        s_ref[s, sender] = jnp.where(valid, scores, NEG)

    def soften(s):
        scores = s_ref[s]
        top = jnp.max(jnp.max(scores, axis=0), axis=-1, keepdims=True)
        weights = jnp.exp(scores - top[None])
        sum_ref[s] = jnp.broadcast_to(jnp.sum(jnp.sum(weights, axis=0), axis=-1, keepdims=True), (q_rows, head))
        p_ref[s] = weights.astype(jnp.bfloat16)

    def values_step(s, sender):
        values = merged(s, sender, vbuf, vnew_ref)
        acc_ref[s] += jnp.dot(p_ref[s, sender], values, preferred_element_type=jnp.float32)

    def each(step):
        def body(s, carry):
            step(s)
            return carry
        lax.fori_loop(0, rows, body, 0)

    own_k.wait()
    each(lambda s: keys_step(s, me))
    for far, other in order:
        sender = device(chips - far if far else 0, other)
        arrival(0, k_hbm, kbuf, sender).wait_recv()
        each(lambda s: keys_step(s, sender))
    each(soften)
    acc_ref[...] = jnp.zeros_like(acc_ref)
    own_v.wait()
    each(lambda s: values_step(s, me))
    wo_copy.wait()
    for far, other in order:
        sender = device(chips - far if far else 0, other)
        arrival(1, v_hbm, vbuf, sender).wait_recv()
        each(lambda s: values_step(s, sender))

    for j in range(heads):
        att_ref[:, j * head:(j + 1) * head] = (acc_ref[:, j, :] / sum_ref[:, j, :]).astype(jnp.bfloat16)
    for copy in sends:
        copy.wait_send()


def finish_kernel(kbuf, vbuf, wo_ref, att_ref, x_ref, y_ref, k_out, v_out, sem):
    rows = kbuf.shape[0]
    copies = [
        pltpu.make_async_copy(src.at[b], dst.at[b], sem.at[i, b])
        for i, (src, dst) in enumerate([(kbuf, k_out), (vbuf, v_out)]) for b in range(rows)
    ]
    for copy in copies:
        copy.start()
    cols = 512
    for c in range(y_ref.shape[1] // cols):
        span = slice(c * cols, (c + 1) * cols)
        out = jnp.dot(att_ref[...], wo_ref[:, span], preferred_element_type=jnp.float32)
        y_ref[:, span] = (x_ref[:, span].astype(jnp.float32) + out).astype(jnp.bfloat16)
    for copy in copies:
        copy.wait()


def solution(mesh):
    n = mesh.shape['cp']
    batch_spec = P(('dp', 'cp'))
    seq_spec = P('dp', 'cp')
    whole = P()
    hbm = pl.BlockSpec(memory_space=pl.ANY)
    vmem = pl.BlockSpec(memory_space=pltpu.VMEM)

    def per_device(x_tok, prompt_lens, k_cache, v_cache, norm_gain, w_q, b_q, w_k, b_k, w_v, b_v, w_o):
        rows, d_model = x_tok.shape
        batch, slots, kv_heads, head = k_cache.shape
        q_cols = w_q.shape[1]
        heads = q_cols // head
        q_rows = -(-heads // PACK) * PACK
        tiles = slots * kv_heads // PACK
        all_tiles = tiles * n
        block_rows = tiles * PACK
        cols = w_k.shape[1]
        half = head // 2
        positions = lax.dynamic_slice_in_dim(prompt_lens, lax.axis_index('cp') * rows, rows)
        inv_freq = jnp.power(ROPE_THETA, -(jnp.arange(half, dtype=jnp.float32) * 2.0 / head))
        angle = positions.astype(jnp.float32)[:, None] * inv_freq
        cos_t, sin_t = jnp.cos(angle), jnp.sin(angle)
        rot = jnp.stack([jnp.concatenate([cos_t, cos_t], -1), jnp.concatenate([-sin_t, sin_t], -1)])

        bf16, f32 = jnp.bfloat16, jnp.float32
        kbuf, vbuf, wo, att = pl.pallas_call(
            functools.partial(gather_kernel, n, kv_heads),
            out_shape=[
                pltpu.VMEM((rows, all_tiles, PACK, head), bf16),
                pltpu.VMEM((rows, all_tiles, PACK, head), bf16),
                pltpu.VMEM(w_o.shape, bf16),
                pltpu.VMEM((rows, q_cols), bf16),
            ],
            in_specs=[hbm] * 13,
            out_specs=[vmem] * 4,
            scratch_shapes=[
                pltpu.SMEM((1, batch), jnp.int32),
                pltpu.VMEM((rows, d_model), bf16),
                pltpu.VMEM((2, rows, head), f32),
                pltpu.VMEM((1, d_model), bf16),
                pltpu.VMEM((1, q_cols), bf16),
                pltpu.VMEM((1, cols), bf16),
                pltpu.VMEM((1, cols), bf16),
                pltpu.VMEM((3, d_model, cols), bf16),
                pltpu.VMEM((rows, d_model), bf16),
                pltpu.VMEM((rows, q_rows, head), f32),
                pltpu.VMEM((rows, PACK, head), f32),
                pltpu.VMEM((rows, PACK, head), f32),
                pltpu.VMEM((rows, n, q_rows, block_rows), f32),
                pltpu.VMEM((rows, n, q_rows, block_rows), bf16),
                pltpu.VMEM((rows, q_rows, head), f32),
                pltpu.VMEM((rows, q_rows, head), f32),
                pltpu.SemaphoreType.DMA((7,)),
                pltpu.SemaphoreType.DMA((3,)),
                pltpu.SemaphoreType.DMA,
                pltpu.SemaphoreType.DMA((2,)),
                pltpu.SemaphoreType.DMA((2, n)),
                pltpu.SemaphoreType.DMA((2, n)),
            ],
            compiler_params=pltpu.CompilerParams(collective_id=0, has_side_effects=True, vmem_limit_bytes=28 * 1024 * 1024),
            name='gather_attend',
        )(prompt_lens[None], x_tok, rot, norm_gain[None], w_q, b_q[None], w_k, b_k[None], w_v, b_v[None], w_o,
          k_cache.reshape(batch, tiles, PACK, head), v_cache.reshape(batch, tiles, PACK, head))

        y_out, k_out, v_out = pl.pallas_call(
            finish_kernel,
            out_shape=[
                jax.ShapeDtypeStruct(x_tok.shape, bf16),
                jax.ShapeDtypeStruct(kbuf.shape, bf16),
                jax.ShapeDtypeStruct(vbuf.shape, bf16),
            ],
            in_specs=[vmem] * 5,
            out_specs=[vmem, hbm, hbm],
            scratch_shapes=[pltpu.SemaphoreType.DMA((2, rows))],
            compiler_params=pltpu.CompilerParams(vmem_limit_bytes=28 * 1024 * 1024),
            name='finish',
        )(*[pltpu.with_memory_space_constraint(a, pltpu.VMEM) for a in (kbuf, vbuf, wo, att)], x_tok)
        shape = (rows, slots * n, kv_heads, head)
        return y_out, k_out.reshape(shape), v_out.reshape(shape)

    return jax.shard_map(per_device, mesh=mesh, in_specs=(batch_spec, P('dp'), seq_spec, seq_spec, whole, whole, whole, whole, whole, whole, whole, whole), out_specs=(batch_spec, batch_spec, batch_spec), check_vma=False)
```

```python
import functools

import jax
import jax.numpy as jnp
import numpy as np
from jax import lax
from jax.experimental import pallas as pl
from jax.experimental.pallas import tpu as pltpu
from jax.sharding import PartitionSpec as P

RMS_EPS = 1e-6
ROPE_THETA = 1000000.0
PACK = 16
NEG = -1e30


def gather_kernel(n, kv_heads, lens_hbm, x_hbm, freq_hbm, gain_hbm, wq_hbm, bq_hbm, wk_hbm, bk_hbm, wv_hbm, bv_hbm, wo_hbm, k_hbm, v_hbm,
                  kbuf, vbuf, wo_ref, att_ref,
                  lens, x_ref, freq_ref, gain_ref, bq_ref, bk_ref, bv_ref, wbuf, h_ref, qf_ref, knew_ref, vnew_ref, s_ref, p_ref, acc_ref, sum_ref,
                  small_sem, wsem, wo_sem, k_send, k_recv, v_send, v_recv):
    rows, d_model = x_ref.shape
    head = acc_ref.shape[-1]
    q_rows = acc_ref.shape[1]
    heads = att_ref.shape[1] // head
    group = heads // kv_heads
    tiles = k_hbm.shape[1]
    block_rows = tiles * PACK
    slots = block_rows // kv_heads
    cols = wbuf.shape[2]
    me = lax.axis_index('cp')

    chip, core = me // 2, lax.rem(me, 2)
    chips = n // 2
    parts = v_recv.shape[1]
    part_rows = rows // parts

    fars = sorted(range(1, chips), key=lambda f: -min(f, chips - f))

    def place(t, way):
        far = sum(jnp.where(t // 2 == k + 1, f, 0) for k, f in enumerate(fars))
        return lax.rem(chip + way * far + chips, chips) * 2 + lax.rem(core + t, 2)

    def block(ref, owner, part, count):
        return ref.at[pl.ds(owner * rows + part * count, count)]

    def span(ref, sender, part, count):
        return ref.at[pl.ds(part * count, count), pl.ds(sender * tiles, tiles)]

    def keys_copy(to, sender):
        return pltpu.make_async_remote_copy(
            src_ref=block(k_hbm, to, 0, rows), dst_ref=span(kbuf, sender, 0, rows), send_sem=k_send.at[to], recv_sem=k_recv.at[sender],
            device_id={'cp': to}, device_id_type=pl.DeviceIdType.MESH)

    def values_copy(to, sender, part):
        return pltpu.make_async_remote_copy(
            src_ref=block(v_hbm, to, part, part_rows), dst_ref=span(vbuf, sender, part, part_rows), send_sem=v_send.at[to, part],
            recv_sem=v_recv.at[sender, part], device_id={'cp': to}, device_id_type=pl.DeviceIdType.MESH)

    barrier = pltpu.get_barrier_semaphore()
    for t in range(1, n):
        pl.semaphore_signal(barrier, inc=1, device_id={'cp': place(t, 1)}, device_id_type=pl.DeviceIdType.MESH)

    smalls = [
        pltpu.make_async_copy(src, dst, small_sem.at[i])
        for i, (src, dst) in enumerate([
            (lens_hbm, lens), (x_hbm, x_ref), (freq_hbm, freq_ref), (gain_hbm, gain_ref), (bq_hbm, bq_ref), (bk_hbm, bk_ref), (bv_hbm, bv_ref)])
    ]
    for copy in smalls:
        copy.start()

    blocks = [(wk_hbm, 0), (wv_hbm, 0)] + [(wq_hbm, c) for c in range(wq_hbm.shape[1] // cols)]

    def weight_copy(t):
        src, c = blocks[t]
        return pltpu.make_async_copy(src.at[:, pl.ds(c * cols, cols)], wbuf.at[t % wbuf.shape[0]], wsem.at[t % wbuf.shape[0]])

    for t in range(wbuf.shape[0]):
        weight_copy(t).start()

    pltpu.make_async_copy(block(k_hbm, me, 0, rows), span(kbuf, me, 0, rows), k_recv.at[me]).start()
    for part in range(parts):
        pltpu.make_async_copy(block(v_hbm, me, part, part_rows), span(vbuf, me, part, part_rows), v_recv.at[me, part]).start()

    pl.semaphore_wait(barrier, n - 1)
    for t in range(1, n):
        keys_copy(place(t, 1), me).start()
    for part in range(parts):
        for t in range(1, n):
            values_copy(place(t, 1), me, part).start()

    for copy in smalls:
        copy.wait()
    x_wide = x_ref[...].astype(jnp.float32)
    mean_sq = jnp.mean(x_wide * x_wide, axis=-1, keepdims=True)
    h_ref[...] = (x_wide * lax.rsqrt(mean_sq + RMS_EPS) * gain_ref[...].astype(jnp.float32)[None]).astype(jnp.bfloat16)
    row = lax.broadcasted_iota(jnp.int32, (rows, head), 0)
    lane = lax.broadcasted_iota(jnp.int32, (rows, head), 1)
    positions = sum(jnp.where(row == b, lens[me * rows + b], 0) for b in range(rows))
    angle = positions.astype(jnp.float32) * freq_ref[...]
    cos_t = jnp.cos(angle)
    sin_t = jnp.where(lane < head // 2, -jnp.sin(angle), jnp.sin(angle))

    def rotate(v):
        return v * cos_t + pltpu.roll(v, head // 2, 1) * sin_t

    qf_ref[...] = jnp.zeros_like(qf_ref)
    for t in range(len(blocks)):
        weight_copy(t).wait()
        out = jnp.dot(h_ref[...], wbuf[t % wbuf.shape[0]], preferred_element_type=jnp.float32)
        if t + wbuf.shape[0] < len(blocks):
            weight_copy(t + wbuf.shape[0]).start()
        c = blocks[t][1]
        bias = (bk_ref if t == 0 else bv_ref if t == 1 else bq_ref)[c * cols:(c + 1) * cols]
        out = out + bias.astype(jnp.float32)[None]
        for i in range(cols // head):
            part = out[:, i * head:(i + 1) * head]
            if t == 0:
                part = rotate(part).astype(jnp.bfloat16).astype(jnp.float32)
                for r in range(PACK // kv_heads):
                    knew_ref[:, r * kv_heads + i, :] = part
            elif t == 1:
                part = part.astype(jnp.bfloat16).astype(jnp.float32)
                for r in range(PACK // kv_heads):
                    vnew_ref[:, r * kv_heads + i, :] = part
            else:
                qf_ref[:, c * (cols // head) + i, :] = rotate(part)
    wo_copy = pltpu.make_async_copy(wo_hbm, wo_ref, wo_sem)
    wo_copy.start()

    def merged(s, sender, buf, new_ref):
        pos = lens[me * rows + s]
        tile = buf[s, pl.ds(sender * tiles, tiles)].astype(jnp.float32)
        shape = (tiles, PACK, head)
        slot = sender * slots + lax.broadcasted_iota(jnp.int32, shape, 0) * (PACK // kv_heads) + lax.broadcasted_iota(jnp.int32, shape, 1) // kv_heads
        new = jnp.broadcast_to(new_ref[s][None], shape)
        tile = jnp.where(slot < pos, tile, jnp.where(slot == pos, new, 0.0)).astype(jnp.bfloat16)
        buf[s, pl.ds(sender * tiles, tiles)] = tile
        return tile.reshape(block_rows, head)

    def keys_step(s, sender):
        pos = lens[me * rows + s]
        keys = merged(s, sender, kbuf, knew_ref)
        query = qf_ref[s].astype(jnp.bfloat16)
        scores = lax.dot_general(query, keys, (((1,), (1,)), ((), ())), preferred_element_type=jnp.float32) * (head ** -0.5)
        row = lax.broadcasted_iota(jnp.int32, scores.shape, 0)
        col = lax.broadcasted_iota(jnp.int32, scores.shape, 1)
        valid = (col % kv_heads == row // group) & (sender * slots + col // kv_heads <= pos)
        s_ref[s, sender] = jnp.where(valid, scores, NEG)
        return 0

    def soften(s):
        scores = s_ref[s]
        top = jnp.max(jnp.max(scores, axis=0), axis=-1, keepdims=True)
        weights = jnp.exp(scores - top[None])
        sum_ref[s] = jnp.broadcast_to(jnp.sum(jnp.sum(weights, axis=0), axis=-1, keepdims=True), (q_rows, head))
        p_ref[s] = weights.astype(jnp.bfloat16)
        return 0

    def values_step(s, sender):
        values = merged(s, sender, vbuf, vnew_ref)
        acc_ref[s] += jnp.dot(p_ref[s, sender], values, preferred_element_type=jnp.float32)
        return 0

    def keys_arrival(t, carry):
        sender = place(t, -1)
        keys_copy(sender, sender).wait_recv()
        return lax.fori_loop(0, rows, lambda s, c: keys_step(s, sender), carry)

    def values_arrival(u, carry):
        part, sender = u // n, place(lax.rem(u, n), -1)
        values_copy(sender, sender, part).wait_recv()
        return lax.fori_loop(part * part_rows, (part + 1) * part_rows, lambda s, c: values_step(s, sender), carry)

    lax.fori_loop(0, n, keys_arrival, 0)
    lax.fori_loop(0, rows, lambda s, c: soften(s), 0)
    acc_ref[...] = jnp.zeros_like(acc_ref)
    wo_copy.wait()
    lax.fori_loop(0, n * parts, values_arrival, 0)

    for j in range(heads):
        att_ref[:, j * head:(j + 1) * head] = (acc_ref[:, j, :] / sum_ref[:, j, :]).astype(jnp.bfloat16)
    for t in range(1, n):
        keys_copy(place(t, 1), me).wait_send()
        for part in range(parts):
            values_copy(place(t, 1), me, part).wait_send()


def finish_kernel(kbuf, vbuf, wo_ref, att_ref, x_ref, y_ref, k_out, v_out, sem):
    rows = kbuf.shape[0]
    copies = [
        pltpu.make_async_copy(src.at[b], dst.at[b], sem.at[i, b])
        for i, (src, dst) in enumerate([(kbuf, k_out), (vbuf, v_out)]) for b in range(rows)
    ]
    for copy in copies:
        copy.start()
    cols = 512

    def project(c, carry):
        span = pl.ds(pl.multiple_of(c * cols, cols), cols)
        out = jnp.dot(att_ref[...], wo_ref[:, span], preferred_element_type=jnp.float32)
        y_ref[:, span] = (x_ref[:, span].astype(jnp.float32) + out).astype(jnp.bfloat16)
        return carry

    lax.fori_loop(0, y_ref.shape[1] // cols, project, 0)
    for copy in copies:
        copy.wait()


def solution(mesh):
    n = mesh.shape['cp']
    batch_spec = P(('dp', 'cp'))
    seq_spec = P('dp', 'cp')
    whole = P()
    hbm = pl.BlockSpec(memory_space=pl.ANY)
    vmem = pl.BlockSpec(memory_space=pltpu.VMEM)

    def per_device(x_tok, prompt_lens, k_cache, v_cache, norm_gain, w_q, b_q, w_k, b_k, w_v, b_v, w_o):
        rows, d_model = x_tok.shape
        batch, slots, kv_heads, head = k_cache.shape
        q_cols = w_q.shape[1]
        heads = q_cols // head
        q_rows = -(-heads // PACK) * PACK
        tiles = slots * kv_heads // PACK
        all_tiles = tiles * n
        block_rows = tiles * PACK
        cols = w_k.shape[1]
        half = head // 2
        freq = np.power(ROPE_THETA, -np.arange(half) * 2.0 / head).astype(np.float32)
        freq = jnp.asarray(np.concatenate([freq, freq])[None])
        parts = 4

        bf16, f32 = jnp.bfloat16, jnp.float32
        kbuf, vbuf, wo, att = pl.pallas_call(
            functools.partial(gather_kernel, n, kv_heads),
            out_shape=[
                pltpu.VMEM((rows, all_tiles, PACK, head), bf16),
                pltpu.VMEM((rows, all_tiles, PACK, head), bf16),
                pltpu.VMEM(w_o.shape, bf16),
                pltpu.VMEM((rows, q_cols), bf16),
            ],
            in_specs=[hbm] * 13,
            out_specs=[vmem] * 4,
            scratch_shapes=[
                pltpu.SMEM((batch,), jnp.int32),
                pltpu.VMEM((rows, d_model), bf16),
                pltpu.VMEM((1, head), f32),
                pltpu.VMEM((d_model,), bf16),
                pltpu.VMEM((q_cols,), bf16),
                pltpu.VMEM((cols,), bf16),
                pltpu.VMEM((cols,), bf16),
                pltpu.VMEM((3, d_model, cols), bf16),
                pltpu.VMEM((rows, d_model), bf16),
                pltpu.VMEM((rows, q_rows, head), f32),
                pltpu.VMEM((rows, PACK, head), f32),
                pltpu.VMEM((rows, PACK, head), f32),
                pltpu.VMEM((rows, n, q_rows, block_rows), f32),
                pltpu.VMEM((rows, n, q_rows, block_rows), bf16),
                pltpu.VMEM((rows, q_rows, head), f32),
                pltpu.VMEM((rows, q_rows, head), f32),
                pltpu.SemaphoreType.DMA((7,)),
                pltpu.SemaphoreType.DMA((3,)),
                pltpu.SemaphoreType.DMA,
                pltpu.SemaphoreType.DMA((n,)),
                pltpu.SemaphoreType.DMA((n,)),
                pltpu.SemaphoreType.DMA((n, parts)),
                pltpu.SemaphoreType.DMA((n, parts)),
            ],
            compiler_params=pltpu.CompilerParams(collective_id=0, has_side_effects=True, vmem_limit_bytes=28 * 1024 * 1024),
            name='gather_attend',
        )(prompt_lens, x_tok, freq, norm_gain, w_q, b_q, w_k, b_k, w_v, b_v, w_o,
          k_cache.reshape(batch, tiles, PACK, head), v_cache.reshape(batch, tiles, PACK, head))

        y_out, k_out, v_out = pl.pallas_call(
            finish_kernel,
            out_shape=[
                jax.ShapeDtypeStruct(x_tok.shape, bf16),
                jax.ShapeDtypeStruct(kbuf.shape, bf16),
                jax.ShapeDtypeStruct(vbuf.shape, bf16),
            ],
            in_specs=[vmem] * 5,
            out_specs=[vmem, hbm, hbm],
            scratch_shapes=[pltpu.SemaphoreType.DMA((2, rows))],
            compiler_params=pltpu.CompilerParams(vmem_limit_bytes=28 * 1024 * 1024),
            name='finish',
        )(*[pltpu.with_memory_space_constraint(a, pltpu.VMEM) for a in (kbuf, vbuf, wo, att)], x_tok)
        shape = (rows, slots * n, kv_heads, head)
        return y_out, k_out.reshape(shape), v_out.reshape(shape)

    return jax.shard_map(per_device, mesh=mesh, in_specs=(batch_spec, P('dp'), seq_spec, seq_spec, whole, whole, whole, whole, whole, whole, whole, whole), out_specs=(batch_spec, batch_spec, batch_spec), check_vma=False)
```

```python
import functools

import jax
import jax.numpy as jnp
import numpy as np
from jax import lax
from jax.experimental import pallas as pl
from jax.experimental.pallas import tpu as pltpu
from jax.sharding import PartitionSpec as P

RMS_EPS = 1e-6
ROPE_THETA = 1000000.0
PACK = 16
NEG = -1e30


def gather_kernel(n, kv_heads, lens_hbm, x_hbm, freq_hbm, gain_hbm, wq_hbm, bq_hbm, wk_hbm, bk_hbm, wv_hbm, bv_hbm, wo_hbm, k_hbm, v_hbm,
                  kbuf, vbuf, wo_ref, att_ref, x_ref,
                  lens, freq_ref, gain_ref, bq_ref, bk_ref, bv_ref, wbuf, h_ref, qf_ref, knew_ref, vnew_ref, s_ref, p_ref, acc_ref, sum_ref,
                  small_sem, wsem, wo_sem, k_send, k_recv, v_send, v_recv):
    rows, d_model = x_ref.shape
    head = acc_ref.shape[-1]
    q_rows = acc_ref.shape[1]
    heads = att_ref.shape[1] // head
    group = heads // kv_heads
    tiles = k_hbm.shape[1]
    block_rows = tiles * PACK
    slots = block_rows // kv_heads
    cols = wbuf.shape[2]
    me = lax.axis_index('cp')

    chip, core = me // 2, lax.rem(me, 2)
    chips = n // 2
    parts = v_recv.shape[1]
    part_rows = rows // parts

    fars = sorted(range(1, chips), key=lambda f: -min(f, chips - f))

    def place(t, way):
        far = sum(jnp.where(t // 2 == k + 1, f, 0) for k, f in enumerate(fars))
        return lax.rem(chip + way * far + chips, chips) * 2 + lax.rem(core + t, 2)

    def block(ref, owner, part, count):
        return ref.at[pl.ds(owner * rows + part * count, count)]

    def span(ref, sender, part, count):
        return ref.at[pl.ds(part * count, count), pl.ds(sender * tiles, tiles)]

    def keys_copy(to, sender):
        return pltpu.make_async_remote_copy(
            src_ref=block(k_hbm, to, 0, rows), dst_ref=span(kbuf, sender, 0, rows), send_sem=k_send.at[to], recv_sem=k_recv.at[sender],
            device_id={'cp': to}, device_id_type=pl.DeviceIdType.MESH)

    def values_copy(to, sender, part):
        return pltpu.make_async_remote_copy(
            src_ref=block(v_hbm, to, part, part_rows), dst_ref=span(vbuf, sender, part, part_rows), send_sem=v_send.at[to, part],
            recv_sem=v_recv.at[sender, part], device_id={'cp': to}, device_id_type=pl.DeviceIdType.MESH)

    barrier = pltpu.get_barrier_semaphore()
    for t in range(1, n):
        pl.semaphore_signal(barrier, inc=1, device_id={'cp': place(t, 1)}, device_id_type=pl.DeviceIdType.MESH)

    smalls = [
        pltpu.make_async_copy(src, dst, small_sem.at[i])
        for i, (src, dst) in enumerate([
            (lens_hbm, lens), (x_hbm, x_ref), (freq_hbm, freq_ref), (gain_hbm, gain_ref), (bq_hbm, bq_ref), (bk_hbm, bk_ref), (bv_hbm, bv_ref)])
    ]
    for copy in smalls:
        copy.start()

    blocks = [(wk_hbm, 0), (wv_hbm, 0)] + [(wq_hbm, c) for c in range(wq_hbm.shape[1] // cols)]

    def weight_copy(t):
        src, c = blocks[t]
        return pltpu.make_async_copy(src.at[:, pl.ds(c * cols, cols)], wbuf.at[t % wbuf.shape[0]], wsem.at[t % wbuf.shape[0]])

    for t in range(wbuf.shape[0]):
        weight_copy(t).start()

    pltpu.make_async_copy(block(k_hbm, me, 0, rows), span(kbuf, me, 0, rows), k_recv.at[me]).start()
    for part in range(parts):
        pltpu.make_async_copy(block(v_hbm, me, part, part_rows), span(vbuf, me, part, part_rows), v_recv.at[me, part]).start()

    pl.semaphore_wait(barrier, n - 1)
    for t in range(1, n):
        keys_copy(place(t, 1), me).start()
    for part in range(parts):
        for t in range(1, n):
            values_copy(place(t, 1), me, part).start()

    for copy in smalls:
        copy.wait()
    x_wide = x_ref[...].astype(jnp.float32)
    mean_sq = jnp.mean(x_wide * x_wide, axis=-1, keepdims=True)
    h_ref[...] = (x_wide * lax.rsqrt(mean_sq + RMS_EPS) * gain_ref[...].astype(jnp.float32)[None]).astype(jnp.bfloat16)
    row = lax.broadcasted_iota(jnp.int32, (rows, head), 0)
    lane = lax.broadcasted_iota(jnp.int32, (rows, head), 1)
    positions = sum(jnp.where(row == b, lens[me * rows + b], 0) for b in range(rows))
    angle = positions.astype(jnp.float32) * freq_ref[...]
    cos_t = jnp.cos(angle)
    sin_t = jnp.where(lane < head // 2, -jnp.sin(angle), jnp.sin(angle))

    def rotate(v):
        return v * cos_t + pltpu.roll(v, head // 2, 1) * sin_t

    qf_ref[...] = jnp.zeros_like(qf_ref)
    for t in range(len(blocks)):
        weight_copy(t).wait()
        out = jnp.dot(h_ref[...], wbuf[t % wbuf.shape[0]], preferred_element_type=jnp.float32)
        if t + wbuf.shape[0] < len(blocks):
            weight_copy(t + wbuf.shape[0]).start()
        c = blocks[t][1]
        bias = (bk_ref if t == 0 else bv_ref if t == 1 else bq_ref)[c * cols:(c + 1) * cols]
        out = out + bias.astype(jnp.float32)[None]
        for i in range(cols // head):
            part = out[:, i * head:(i + 1) * head]
            if t == 0:
                part = rotate(part).astype(jnp.bfloat16).astype(jnp.float32)
                for r in range(PACK // kv_heads):
                    knew_ref[:, r * kv_heads + i, :] = part
            elif t == 1:
                part = part.astype(jnp.bfloat16).astype(jnp.float32)
                for r in range(PACK // kv_heads):
                    vnew_ref[:, r * kv_heads + i, :] = part
            else:
                qf_ref[:, c * (cols // head) + i, :] = rotate(part)
    wo_copy = pltpu.make_async_copy(wo_hbm, wo_ref, wo_sem)
    wo_copy.start()

    def merged(s, sender, buf, new_ref):
        pos = lens[me * rows + s]
        tile = buf[s, pl.ds(sender * tiles, tiles)].astype(jnp.float32)
        shape = (tiles, PACK, head)
        slot = sender * slots + lax.broadcasted_iota(jnp.int32, shape, 0) * (PACK // kv_heads) + lax.broadcasted_iota(jnp.int32, shape, 1) // kv_heads
        new = jnp.broadcast_to(new_ref[s][None], shape)
        tile = jnp.where(slot < pos, tile, jnp.where(slot == pos, new, 0.0)).astype(jnp.bfloat16)
        buf[s, pl.ds(sender * tiles, tiles)] = tile
        return tile.reshape(block_rows, head)

    def keys_step(s, sender):
        pos = lens[me * rows + s]
        keys = merged(s, sender, kbuf, knew_ref)
        query = qf_ref[s].astype(jnp.bfloat16)
        scores = lax.dot_general(query, keys, (((1,), (1,)), ((), ())), preferred_element_type=jnp.float32) * (head ** -0.5)
        row = lax.broadcasted_iota(jnp.int32, scores.shape, 0)
        col = lax.broadcasted_iota(jnp.int32, scores.shape, 1)
        valid = (col % kv_heads == row // group) & (sender * slots + col // kv_heads <= pos)
        s_ref[s, sender] = jnp.where(valid, scores, NEG)
        return 0

    def soften(s):
        scores = s_ref[s]
        top = jnp.max(jnp.max(scores, axis=0), axis=-1, keepdims=True)
        weights = jnp.exp(scores - top[None])
        sum_ref[s] = jnp.broadcast_to(jnp.sum(jnp.sum(weights, axis=0), axis=-1, keepdims=True), (q_rows, head))
        p_ref[s] = weights.astype(jnp.bfloat16)
        return 0

    def values_step(s, sender):
        values = merged(s, sender, vbuf, vnew_ref)
        acc_ref[s] += jnp.dot(p_ref[s, sender], values, preferred_element_type=jnp.float32)
        return 0

    def keys_arrival(t, carry):
        sender = place(t, -1)
        keys_copy(sender, sender).wait_recv()
        return lax.fori_loop(0, rows, lambda s, c: keys_step(s, sender), carry)

    def values_arrival(u, carry):
        part, sender = u // n, place(lax.rem(u, n), -1)
        values_copy(sender, sender, part).wait_recv()
        return lax.fori_loop(part * part_rows, (part + 1) * part_rows, lambda s, c: values_step(s, sender), carry)

    lax.fori_loop(0, n, keys_arrival, 0)
    lax.fori_loop(0, rows, lambda s, c: soften(s), 0)
    acc_ref[...] = jnp.zeros_like(acc_ref)
    wo_copy.wait()
    lax.fori_loop(0, n * parts, values_arrival, 0)

    for j in range(heads):
        att_ref[:, j * head:(j + 1) * head] = (acc_ref[:, j, :] / sum_ref[:, j, :]).astype(jnp.bfloat16)
    for t in range(1, n):
        keys_copy(place(t, 1), me).wait_send()
        for part in range(parts):
            values_copy(place(t, 1), me, part).wait_send()


def finish_kernel(kbuf, vbuf, wo_ref, att_ref, x_ref, y_out, k_out, v_out, y_ref, sem, y_sem):
    rows = kbuf.shape[0]
    copies = [
        pltpu.make_async_copy(src.at[b], dst.at[b], sem.at[i, b])
        for i, (src, dst) in enumerate([(kbuf, k_out), (vbuf, v_out)]) for b in range(rows)
    ]
    for copy in copies:
        copy.start()
    cols = 512

    def project(c, carry):
        span = pl.ds(pl.multiple_of(c * cols, cols), cols)
        out = jnp.dot(att_ref[...], wo_ref[:, span], preferred_element_type=jnp.float32)
        y_ref[:, span] = (x_ref[:, span].astype(jnp.float32) + out).astype(jnp.bfloat16)
        return carry

    lax.fori_loop(0, y_ref.shape[1] // cols, project, 0)
    y_copy = pltpu.make_async_copy(y_ref, y_out, y_sem)
    y_copy.start()
    for copy in copies:
        copy.wait()
    y_copy.wait()


def solution(mesh):
    n = mesh.shape['cp']
    batch_spec = P(('dp', 'cp'))
    seq_spec = P('dp', 'cp')
    whole = P()
    hbm = pl.BlockSpec(memory_space=pl.ANY)
    vmem = pl.BlockSpec(memory_space=pltpu.VMEM)

    def per_device(x_tok, prompt_lens, k_cache, v_cache, norm_gain, w_q, b_q, w_k, b_k, w_v, b_v, w_o):
        rows, d_model = x_tok.shape
        batch, slots, kv_heads, head = k_cache.shape
        q_cols = w_q.shape[1]
        heads = q_cols // head
        q_rows = -(-heads // PACK) * PACK
        tiles = slots * kv_heads // PACK
        all_tiles = tiles * n
        block_rows = tiles * PACK
        cols = w_k.shape[1]
        half = head // 2
        freq = np.power(ROPE_THETA, -np.arange(half) * 2.0 / head).astype(np.float32)
        freq = jnp.asarray(np.concatenate([freq, freq])[None])
        parts = 4

        bf16, f32 = jnp.bfloat16, jnp.float32
        kbuf, vbuf, wo, att, x_near = pl.pallas_call(
            functools.partial(gather_kernel, n, kv_heads),
            out_shape=[
                pltpu.VMEM((rows, all_tiles, PACK, head), bf16),
                pltpu.VMEM((rows, all_tiles, PACK, head), bf16),
                pltpu.VMEM(w_o.shape, bf16),
                pltpu.VMEM((rows, q_cols), bf16),
                pltpu.VMEM((rows, d_model), bf16),
            ],
            in_specs=[hbm] * 13,
            out_specs=[vmem] * 5,
            scratch_shapes=[
                pltpu.SMEM((batch,), jnp.int32),
                pltpu.VMEM((1, head), f32),
                pltpu.VMEM((d_model,), bf16),
                pltpu.VMEM((q_cols,), bf16),
                pltpu.VMEM((cols,), bf16),
                pltpu.VMEM((cols,), bf16),
                pltpu.VMEM((3, d_model, cols), bf16),
                pltpu.VMEM((rows, d_model), bf16),
                pltpu.VMEM((rows, q_rows, head), f32),
                pltpu.VMEM((rows, PACK, head), f32),
                pltpu.VMEM((rows, PACK, head), f32),
                pltpu.VMEM((rows, n, q_rows, block_rows), f32),
                pltpu.VMEM((rows, n, q_rows, block_rows), bf16),
                pltpu.VMEM((rows, q_rows, head), f32),
                pltpu.VMEM((rows, q_rows, head), f32),
                pltpu.SemaphoreType.DMA((7,)),
                pltpu.SemaphoreType.DMA((3,)),
                pltpu.SemaphoreType.DMA,
                pltpu.SemaphoreType.DMA((n,)),
                pltpu.SemaphoreType.DMA((n,)),
                pltpu.SemaphoreType.DMA((n, parts)),
                pltpu.SemaphoreType.DMA((n, parts)),
            ],
            compiler_params=pltpu.CompilerParams(collective_id=0, has_side_effects=True, vmem_limit_bytes=28 * 1024 * 1024),
            name='gather_attend',
        )(prompt_lens, x_tok, freq, norm_gain, w_q, b_q, w_k, b_k, w_v, b_v, w_o,
          k_cache.reshape(batch, tiles, PACK, head), v_cache.reshape(batch, tiles, PACK, head))

        y_out, k_out, v_out = pl.pallas_call(
            finish_kernel,
            out_shape=[
                jax.ShapeDtypeStruct(x_tok.shape, bf16),
                jax.ShapeDtypeStruct(kbuf.shape, bf16),
                jax.ShapeDtypeStruct(vbuf.shape, bf16),
            ],
            in_specs=[vmem] * 5,
            out_specs=[hbm] * 3,
            scratch_shapes=[pltpu.VMEM(x_tok.shape, bf16), pltpu.SemaphoreType.DMA((2, rows)), pltpu.SemaphoreType.DMA],
            compiler_params=pltpu.CompilerParams(vmem_limit_bytes=28 * 1024 * 1024),
            name='finish',
        )(*[pltpu.with_memory_space_constraint(a, pltpu.VMEM) for a in (kbuf, vbuf, wo, att, x_near)])
        shape = (rows, slots * n, kv_heads, head)
        return y_out, k_out.reshape(shape), v_out.reshape(shape)

    return jax.shard_map(per_device, mesh=mesh, in_specs=(batch_spec, P('dp'), seq_spec, seq_spec, whole, whole, whole, whole, whole, whole, whole, whole), out_specs=(batch_spec, batch_spec, batch_spec), check_vma=False)
```

```python
import functools

import jax
import jax.numpy as jnp
import numpy as np
from jax import lax
from jax.experimental import pallas as pl
from jax.experimental.pallas import tpu as pltpu
from jax.sharding import PartitionSpec as P

RMS_EPS = 1e-6
ROPE_THETA = 1000000.0
PACK = 16
NEG = -1e30


def gather_kernel(n, kv_heads, lens_hbm, x_hbm, freq_hbm, gain_hbm, wq_hbm, bq_hbm, wk_hbm, bk_hbm, wv_hbm, bv_hbm, wo_hbm, k_hbm, v_hbm,
                  kbuf, vbuf, wo_ref, att_ref, x_ref,
                  lens, freq_ref, gain_ref, bq_ref, bk_ref, bv_ref, wbuf, k_near, v_near, h_ref, qf_ref, knew_ref, vnew_ref, s_ref, p_ref, acc_ref, sum_ref,
                  small_sem, wsem, wo_sem, near_sem, k_send, k_recv, v_send, v_recv):
    rows, d_model = x_ref.shape
    head = acc_ref.shape[-1]
    q_rows = acc_ref.shape[1]
    heads = att_ref.shape[1] // head
    group = heads // kv_heads
    tiles = k_hbm.shape[1]
    block_rows = tiles * PACK
    slots = block_rows // kv_heads
    cols = wbuf.shape[2]
    me = lax.axis_index('cp')

    chip, core = me // 2, lax.rem(me, 2)
    chips = n // 2
    parts = v_recv.shape[1]
    part_rows = rows // parts

    fars = sorted(range(1, chips), key=lambda f: -min(f, chips - f))

    def place(t, way):
        far = sum(jnp.where(t // 2 == k + 1, f, 0) for k, f in enumerate(fars))
        return lax.rem(chip + way * far + chips, chips) * 2 + lax.rem(core + t, 2)

    def block(ref, owner, part, count):
        return ref.at[pl.ds(owner * rows + part * count, count)]

    def span(ref, sender, part, count):
        return ref.at[pl.ds(part * count, count), pl.ds(sender * tiles, tiles)]

    def keys_copy(to, sender):
        return pltpu.make_async_remote_copy(
            src_ref=block(k_near, to, 0, rows), dst_ref=span(kbuf, sender, 0, rows), send_sem=k_send.at[to], recv_sem=k_recv.at[sender],
            device_id={'cp': to}, device_id_type=pl.DeviceIdType.MESH)

    def values_copy(to, sender, part):
        return pltpu.make_async_remote_copy(
            src_ref=block(v_near, to, part, part_rows), dst_ref=span(vbuf, sender, part, part_rows), send_sem=v_send.at[to, part],
            recv_sem=v_recv.at[sender, part], device_id={'cp': to}, device_id_type=pl.DeviceIdType.MESH)

    barrier = pltpu.get_barrier_semaphore()
    for t in range(1, n):
        pl.semaphore_signal(barrier, inc=1, device_id={'cp': place(t, 1)}, device_id_type=pl.DeviceIdType.MESH)

    def stage(which, to):
        src, dst = ((k_hbm, k_near), (v_hbm, v_near))[which]
        return pltpu.make_async_copy(block(src, to, 0, rows), block(dst, to, 0, rows), near_sem.at[which, to])

    for t in range(1, n):
        stage(0, place(t, 1)).start()

    smalls = [
        pltpu.make_async_copy(src, dst, small_sem.at[i])
        for i, (src, dst) in enumerate([
            (lens_hbm, lens), (x_hbm, x_ref), (freq_hbm, freq_ref), (gain_hbm, gain_ref), (bq_hbm, bq_ref), (bk_hbm, bk_ref), (bv_hbm, bv_ref)])
    ]
    for copy in smalls:
        copy.start()

    blocks = [(wk_hbm, 0), (wv_hbm, 0)] + [(wq_hbm, c) for c in range(wq_hbm.shape[1] // cols)]

    def weight_copy(t):
        src, c = blocks[t]
        return pltpu.make_async_copy(src.at[:, pl.ds(c * cols, cols)], wbuf.at[t % wbuf.shape[0]], wsem.at[t % wbuf.shape[0]])

    pltpu.make_async_copy(block(k_hbm, me, 0, rows), span(kbuf, me, 0, rows), k_recv.at[me]).start()
    for t in range(1, n):
        stage(1, place(t, 1)).start()
    for t in range(wbuf.shape[0]):
        weight_copy(t).start()
    for part in range(parts):
        pltpu.make_async_copy(block(v_hbm, me, part, part_rows), span(vbuf, me, part, part_rows), v_recv.at[me, part]).start()

    pl.semaphore_wait(barrier, n - 1)
    for t in range(1, n):
        stage(0, place(t, 1)).wait()
        keys_copy(place(t, 1), me).start()
    for t in range(1, n):
        stage(1, place(t, 1)).wait()
    for part in range(parts):
        for t in range(1, n):
            values_copy(place(t, 1), me, part).start()

    for copy in smalls:
        copy.wait()
    x_wide = x_ref[...].astype(jnp.float32)
    mean_sq = jnp.mean(x_wide * x_wide, axis=-1, keepdims=True)
    h_ref[...] = (x_wide * lax.rsqrt(mean_sq + RMS_EPS) * gain_ref[...].astype(jnp.float32)[None]).astype(jnp.bfloat16)
    row = lax.broadcasted_iota(jnp.int32, (rows, head), 0)
    lane = lax.broadcasted_iota(jnp.int32, (rows, head), 1)
    positions = sum(jnp.where(row == b, lens[me * rows + b], 0) for b in range(rows))
    angle = positions.astype(jnp.float32) * freq_ref[...]
    cos_t = jnp.cos(angle)
    sin_t = jnp.where(lane < head // 2, -jnp.sin(angle), jnp.sin(angle))

    def rotate(v):
        return v * cos_t + pltpu.roll(v, head // 2, 1) * sin_t

    qf_ref[...] = jnp.zeros_like(qf_ref)
    for t in range(len(blocks)):
        weight_copy(t).wait()
        out = jnp.dot(h_ref[...], wbuf[t % wbuf.shape[0]], preferred_element_type=jnp.float32)
        if t + wbuf.shape[0] < len(blocks):
            weight_copy(t + wbuf.shape[0]).start()
        c = blocks[t][1]
        bias = (bk_ref if t == 0 else bv_ref if t == 1 else bq_ref)[c * cols:(c + 1) * cols]
        out = out + bias.astype(jnp.float32)[None]
        for i in range(cols // head):
            part = out[:, i * head:(i + 1) * head]
            if t == 0:
                part = rotate(part).astype(jnp.bfloat16).astype(jnp.float32)
                for r in range(PACK // kv_heads):
                    knew_ref[:, r * kv_heads + i, :] = part
            elif t == 1:
                part = part.astype(jnp.bfloat16).astype(jnp.float32)
                for r in range(PACK // kv_heads):
                    vnew_ref[:, r * kv_heads + i, :] = part
            else:
                qf_ref[:, c * (cols // head) + i, :] = rotate(part)
    wo_copy = pltpu.make_async_copy(wo_hbm, wo_ref, wo_sem)
    wo_copy.start()

    def merged(s, sender, buf, new_ref):
        pos = lens[me * rows + s]
        tile = buf[s, pl.ds(sender * tiles, tiles)].astype(jnp.float32)
        shape = (tiles, PACK, head)
        slot = sender * slots + lax.broadcasted_iota(jnp.int32, shape, 0) * (PACK // kv_heads) + lax.broadcasted_iota(jnp.int32, shape, 1) // kv_heads
        new = jnp.broadcast_to(new_ref[s][None], shape)
        tile = jnp.where(slot < pos, tile, jnp.where(slot == pos, new, 0.0)).astype(jnp.bfloat16)
        buf[s, pl.ds(sender * tiles, tiles)] = tile
        return tile.reshape(block_rows, head)

    def keys_step(s, sender):
        pos = lens[me * rows + s]
        keys = merged(s, sender, kbuf, knew_ref)
        query = qf_ref[s].astype(jnp.bfloat16)
        scores = lax.dot_general(query, keys, (((1,), (1,)), ((), ())), preferred_element_type=jnp.float32) * (head ** -0.5)
        row = lax.broadcasted_iota(jnp.int32, scores.shape, 0)
        col = lax.broadcasted_iota(jnp.int32, scores.shape, 1)
        valid = (col % kv_heads == row // group) & (sender * slots + col // kv_heads <= pos)
        s_ref[s, sender] = jnp.where(valid, scores, NEG)
        return 0

    def soften(s):
        scores = s_ref[s]
        top = jnp.max(jnp.max(scores, axis=0), axis=-1, keepdims=True)
        weights = jnp.exp(scores - top[None])
        sum_ref[s] = jnp.broadcast_to(jnp.sum(jnp.sum(weights, axis=0), axis=-1, keepdims=True), (q_rows, head))
        p_ref[s] = weights.astype(jnp.bfloat16)
        return 0

    def values_step(s, sender):
        values = merged(s, sender, vbuf, vnew_ref)
        acc_ref[s] += jnp.dot(p_ref[s, sender], values, preferred_element_type=jnp.float32)
        return 0

    def keys_arrival(t, carry):
        sender = place(t, -1)
        keys_copy(sender, sender).wait_recv()
        return lax.fori_loop(0, rows, lambda s, c: keys_step(s, sender), carry)

    def values_arrival(u, carry):
        part, sender = u // n, place(lax.rem(u, n), -1)
        values_copy(sender, sender, part).wait_recv()
        return lax.fori_loop(part * part_rows, (part + 1) * part_rows, lambda s, c: values_step(s, sender), carry)

    lax.fori_loop(0, n, keys_arrival, 0)
    lax.fori_loop(0, rows, lambda s, c: soften(s), 0)
    acc_ref[...] = jnp.zeros_like(acc_ref)
    wo_copy.wait()
    lax.fori_loop(0, n * parts, values_arrival, 0)

    for j in range(heads):
        att_ref[:, j * head:(j + 1) * head] = (acc_ref[:, j, :] / sum_ref[:, j, :]).astype(jnp.bfloat16)
    for t in range(1, n):
        keys_copy(place(t, 1), me).wait_send()
        for part in range(parts):
            values_copy(place(t, 1), me, part).wait_send()


def finish_kernel(kbuf, vbuf, wo_ref, att_ref, x_ref, y_out, k_out, v_out, y_ref, sem, y_sem):
    rows = kbuf.shape[0]
    copies = [
        pltpu.make_async_copy(src.at[b], dst.at[b], sem.at[i, b])
        for i, (src, dst) in enumerate([(kbuf, k_out), (vbuf, v_out)]) for b in range(rows)
    ]
    for copy in copies:
        copy.start()
    cols = 512

    def project(c, carry):
        span = pl.ds(pl.multiple_of(c * cols, cols), cols)
        out = jnp.dot(att_ref[...], wo_ref[:, span], preferred_element_type=jnp.float32)
        y_ref[:, span] = (x_ref[:, span].astype(jnp.float32) + out).astype(jnp.bfloat16)
        return carry

    lax.fori_loop(0, y_ref.shape[1] // cols, project, 0)
    y_copy = pltpu.make_async_copy(y_ref, y_out, y_sem)
    y_copy.start()
    for copy in copies:
        copy.wait()
    y_copy.wait()


def solution(mesh):
    n = mesh.shape['cp']
    batch_spec = P(('dp', 'cp'))
    seq_spec = P('dp', 'cp')
    whole = P()
    hbm = pl.BlockSpec(memory_space=pl.ANY)
    vmem = pl.BlockSpec(memory_space=pltpu.VMEM)

    def per_device(x_tok, prompt_lens, k_cache, v_cache, norm_gain, w_q, b_q, w_k, b_k, w_v, b_v, w_o):
        rows, d_model = x_tok.shape
        batch, slots, kv_heads, head = k_cache.shape
        q_cols = w_q.shape[1]
        heads = q_cols // head
        q_rows = -(-heads // PACK) * PACK
        tiles = slots * kv_heads // PACK
        all_tiles = tiles * n
        block_rows = tiles * PACK
        cols = w_k.shape[1]
        half = head // 2
        freq = np.power(ROPE_THETA, -np.arange(half) * 2.0 / head).astype(np.float32)
        freq = jnp.asarray(np.concatenate([freq, freq])[None])
        parts = rows

        bf16, f32 = jnp.bfloat16, jnp.float32
        kbuf, vbuf, wo, att, x_near = pl.pallas_call(
            functools.partial(gather_kernel, n, kv_heads),
            out_shape=[
                pltpu.VMEM((rows, all_tiles, PACK, head), bf16),
                pltpu.VMEM((rows, all_tiles, PACK, head), bf16),
                pltpu.VMEM(w_o.shape, bf16),
                pltpu.VMEM((rows, q_cols), bf16),
                pltpu.VMEM((rows, d_model), bf16),
            ],
            in_specs=[hbm] * 13,
            out_specs=[vmem] * 5,
            scratch_shapes=[
                pltpu.SMEM((batch,), jnp.int32),
                pltpu.VMEM((1, head), f32),
                pltpu.VMEM((d_model,), bf16),
                pltpu.VMEM((q_cols,), bf16),
                pltpu.VMEM((cols,), bf16),
                pltpu.VMEM((cols,), bf16),
                pltpu.VMEM((3, d_model, cols), bf16),
                pltpu.VMEM((batch, tiles, PACK, head), bf16),
                pltpu.VMEM((batch, tiles, PACK, head), bf16),
                pltpu.VMEM((rows, d_model), bf16),
                pltpu.VMEM((rows, q_rows, head), f32),
                pltpu.VMEM((rows, PACK, head), f32),
                pltpu.VMEM((rows, PACK, head), f32),
                pltpu.VMEM((rows, n, q_rows, block_rows), f32),
                pltpu.VMEM((rows, n, q_rows, block_rows), bf16),
                pltpu.VMEM((rows, q_rows, head), f32),
                pltpu.VMEM((rows, q_rows, head), f32),
                pltpu.SemaphoreType.DMA((7,)),
                pltpu.SemaphoreType.DMA((3,)),
                pltpu.SemaphoreType.DMA,
                pltpu.SemaphoreType.DMA((2, n)),
                pltpu.SemaphoreType.DMA((n,)),
                pltpu.SemaphoreType.DMA((n,)),
                pltpu.SemaphoreType.DMA((n, parts)),
                pltpu.SemaphoreType.DMA((n, parts)),
            ],
            compiler_params=pltpu.CompilerParams(collective_id=0, has_side_effects=True, vmem_limit_bytes=28 * 1024 * 1024),
            name='gather_attend',
        )(prompt_lens, x_tok, freq, norm_gain, w_q, b_q, w_k, b_k, w_v, b_v, w_o,
          k_cache.reshape(batch, tiles, PACK, head), v_cache.reshape(batch, tiles, PACK, head))

        y_out, k_out, v_out = pl.pallas_call(
            finish_kernel,
            out_shape=[
                jax.ShapeDtypeStruct(x_tok.shape, bf16),
                jax.ShapeDtypeStruct(kbuf.shape, bf16),
                jax.ShapeDtypeStruct(vbuf.shape, bf16),
            ],
            in_specs=[vmem] * 5,
            out_specs=[hbm] * 3,
            scratch_shapes=[pltpu.VMEM(x_tok.shape, bf16), pltpu.SemaphoreType.DMA((2, rows)), pltpu.SemaphoreType.DMA],
            compiler_params=pltpu.CompilerParams(vmem_limit_bytes=28 * 1024 * 1024),
            name='finish',
        )(*[pltpu.with_memory_space_constraint(a, pltpu.VMEM) for a in (kbuf, vbuf, wo, att, x_near)])
        shape = (rows, slots * n, kv_heads, head)
        return y_out, k_out.reshape(shape), v_out.reshape(shape)

    return jax.shard_map(per_device, mesh=mesh, in_specs=(batch_spec, P('dp'), seq_spec, seq_spec, whole, whole, whole, whole, whole, whole, whole, whole), out_specs=(batch_spec, batch_spec, batch_spec), check_vma=False)
```

```python
import functools

import jax
import jax.numpy as jnp
import numpy as np
from jax import lax
from jax.experimental import pallas as pl
from jax.experimental.pallas import tpu as pltpu
from jax.sharding import PartitionSpec as P

RMS_EPS = 1e-6
ROPE_THETA = 1000000.0
PACK = 16
NEG = -1e30


def gather_kernel(n, kv_heads, lens_hbm, x_hbm, freq_hbm, gain_hbm, wq_hbm, bq_hbm, wk_hbm, bk_hbm, wv_hbm, bv_hbm, wo_hbm, k_hbm, v_hbm,
                  kbuf, vbuf, wo_ref, att_ref, x_ref,
                  lens, freq_ref, gain_ref, bq_ref, bk_ref, bv_ref, wbuf, h_ref, qf_ref, knew_ref, vnew_ref, s_ref, p_ref, acc_ref, sum_ref,
                  small_sem, wsem, wo_sem, k_send, k_recv, v_send, v_recv):
    rows, d_model = x_ref.shape
    head = acc_ref.shape[-1]
    q_rows = acc_ref.shape[1]
    heads = att_ref.shape[1] // head
    group = heads // kv_heads
    tiles = k_hbm.shape[1]
    block_rows = tiles * PACK
    slots = block_rows // kv_heads
    cols = wbuf.shape[2]
    me = lax.axis_index('cp')

    chip, core = me // 2, lax.rem(me, 2)
    chips = n // 2
    parts = v_recv.shape[1]
    part_rows = rows // parts

    fars = sorted(range(1, chips), key=lambda f: -min(f, chips - f))

    def place(t, way):
        far = sum(jnp.where(t // 2 == k + 1, f, 0) for k, f in enumerate(fars))
        return lax.rem(chip + way * far + chips, chips) * 2 + lax.rem(core + t, 2)

    def block(ref, owner, part, count):
        return ref.at[pl.ds(owner * rows + part * count, count)]

    def span(ref, sender, part, count):
        return ref.at[pl.ds(part * count, count), pl.ds(sender * tiles, tiles)]

    def keys_copy(to, sender):
        return pltpu.make_async_remote_copy(
            src_ref=block(k_hbm, to, 0, rows), dst_ref=span(kbuf, sender, 0, rows), send_sem=k_send.at[to], recv_sem=k_recv.at[sender],
            device_id={'cp': to}, device_id_type=pl.DeviceIdType.MESH)

    def values_copy(to, sender, part):
        return pltpu.make_async_remote_copy(
            src_ref=block(v_hbm, to, part, part_rows), dst_ref=span(vbuf, sender, part, part_rows), send_sem=v_send.at[to, part],
            recv_sem=v_recv.at[sender, part], device_id={'cp': to}, device_id_type=pl.DeviceIdType.MESH)

    barrier = pltpu.get_barrier_semaphore()
    for t in range(1, n):
        pl.semaphore_signal(barrier, inc=1, device_id={'cp': place(t, 1)}, device_id_type=pl.DeviceIdType.MESH)

    smalls = [
        pltpu.make_async_copy(src, dst, small_sem.at[i])
        for i, (src, dst) in enumerate([
            (lens_hbm, lens), (x_hbm, x_ref), (freq_hbm, freq_ref), (gain_hbm, gain_ref), (bq_hbm, bq_ref), (bk_hbm, bk_ref), (bv_hbm, bv_ref)])
    ]
    for copy in smalls:
        copy.start()

    blocks = [(wk_hbm, 0), (wv_hbm, 0)] + [(wq_hbm, c) for c in range(wq_hbm.shape[1] // cols)]

    def weight_copy(t):
        src, c = blocks[t]
        return pltpu.make_async_copy(src.at[:, pl.ds(c * cols, cols)], wbuf.at[t % wbuf.shape[0]], wsem.at[t % wbuf.shape[0]])

    pltpu.make_async_copy(block(k_hbm, me, 0, rows), span(kbuf, me, 0, rows), k_recv.at[me]).start()
    for part in range(parts):
        pltpu.make_async_copy(block(v_hbm, me, part, part_rows), span(vbuf, me, part, part_rows), v_recv.at[me, part]).start()

    pl.semaphore_wait(barrier, n - 1)
    for t in range(1, n):
        keys_copy(place(t, 1), me).start()
    for part in range(parts):
        for t in range(1, n):
            values_copy(place(t, 1), me, part).start()

    for t in range(wbuf.shape[0]):
        weight_copy(t).start()

    for copy in smalls:
        copy.wait()
    x_wide = x_ref[...].astype(jnp.float32)
    mean_sq = jnp.mean(x_wide * x_wide, axis=-1, keepdims=True)
    h_ref[...] = (x_wide * lax.rsqrt(mean_sq + RMS_EPS) * gain_ref[...].astype(jnp.float32)[None]).astype(jnp.bfloat16)
    row = lax.broadcasted_iota(jnp.int32, (rows, head), 0)
    lane = lax.broadcasted_iota(jnp.int32, (rows, head), 1)
    positions = sum(jnp.where(row == b, lens[me * rows + b], 0) for b in range(rows))
    angle = positions.astype(jnp.float32) * freq_ref[...]
    cos_t = jnp.cos(angle)
    sin_t = jnp.where(lane < head // 2, -jnp.sin(angle), jnp.sin(angle))

    def rotate(v):
        return v * cos_t + pltpu.roll(v, head // 2, 1) * sin_t

    qf_ref[...] = jnp.zeros_like(qf_ref)
    for t in range(len(blocks)):
        weight_copy(t).wait()
        out = jnp.dot(h_ref[...], wbuf[t % wbuf.shape[0]], preferred_element_type=jnp.float32)
        if t + wbuf.shape[0] < len(blocks):
            weight_copy(t + wbuf.shape[0]).start()
        c = blocks[t][1]
        bias = (bk_ref if t == 0 else bv_ref if t == 1 else bq_ref)[c * cols:(c + 1) * cols]
        out = out + bias.astype(jnp.float32)[None]
        for i in range(cols // head):
            part = out[:, i * head:(i + 1) * head]
            if t == 0:
                part = rotate(part).astype(jnp.bfloat16).astype(jnp.float32)
                for r in range(PACK // kv_heads):
                    knew_ref[:, r * kv_heads + i, :] = part
            elif t == 1:
                part = part.astype(jnp.bfloat16).astype(jnp.float32)
                for r in range(PACK // kv_heads):
                    vnew_ref[:, r * kv_heads + i, :] = part
            else:
                qf_ref[:, c * (cols // head) + i, :] = rotate(part)
    wo_copy = pltpu.make_async_copy(wo_hbm, wo_ref, wo_sem)
    wo_copy.start()

    def merged(s, sender, buf, new_ref):
        pos = lens[me * rows + s]
        tile = buf[s, pl.ds(sender * tiles, tiles)].astype(jnp.float32)
        shape = (tiles, PACK, head)
        slot = sender * slots + lax.broadcasted_iota(jnp.int32, shape, 0) * (PACK // kv_heads) + lax.broadcasted_iota(jnp.int32, shape, 1) // kv_heads
        new = jnp.broadcast_to(new_ref[s][None], shape)
        tile = jnp.where(slot < pos, tile, jnp.where(slot == pos, new, 0.0)).astype(jnp.bfloat16)
        buf[s, pl.ds(sender * tiles, tiles)] = tile
        return tile.reshape(block_rows, head)

    def keys_step(s, sender):
        pos = lens[me * rows + s]
        keys = merged(s, sender, kbuf, knew_ref)
        query = qf_ref[s].astype(jnp.bfloat16)
        scores = lax.dot_general(query, keys, (((1,), (1,)), ((), ())), preferred_element_type=jnp.float32) * (head ** -0.5)
        row = lax.broadcasted_iota(jnp.int32, scores.shape, 0)
        col = lax.broadcasted_iota(jnp.int32, scores.shape, 1)
        valid = (col % kv_heads == row // group) & (sender * slots + col // kv_heads <= pos)
        s_ref[s, sender] = jnp.where(valid, scores, NEG)
        return 0

    def soften(s):
        scores = s_ref[s]
        top = jnp.max(jnp.max(scores, axis=0), axis=-1, keepdims=True)
        weights = jnp.exp(scores - top[None])
        sum_ref[s] = jnp.broadcast_to(jnp.sum(jnp.sum(weights, axis=0), axis=-1, keepdims=True), (q_rows, head))
        p_ref[s] = weights.astype(jnp.bfloat16)
        return 0

    def values_step(s, sender):
        values = merged(s, sender, vbuf, vnew_ref)
        acc_ref[s] += jnp.dot(p_ref[s, sender], values, preferred_element_type=jnp.float32)
        return 0

    def keys_arrival(t, carry):
        sender = place(t, -1)
        keys_copy(sender, sender).wait_recv()
        return lax.fori_loop(0, rows, lambda s, c: keys_step(s, sender), carry)

    def values_arrival(u, carry):
        part, sender = u // n, place(lax.rem(u, n), -1)
        values_copy(sender, sender, part).wait_recv()
        return lax.fori_loop(part * part_rows, (part + 1) * part_rows, lambda s, c: values_step(s, sender), carry)

    lax.fori_loop(0, n, keys_arrival, 0)
    lax.fori_loop(0, rows, lambda s, c: soften(s), 0)
    acc_ref[...] = jnp.zeros_like(acc_ref)
    wo_copy.wait()
    lax.fori_loop(0, n * parts, values_arrival, 0)

    for j in range(heads):
        att_ref[:, j * head:(j + 1) * head] = (acc_ref[:, j, :] / sum_ref[:, j, :]).astype(jnp.bfloat16)
    for t in range(1, n):
        keys_copy(place(t, 1), me).wait_send()
        for part in range(parts):
            values_copy(place(t, 1), me, part).wait_send()


def finish_kernel(kbuf, vbuf, wo_ref, att_ref, x_ref, y_out, k_out, v_out, y_ref, sem, y_sem):
    rows = kbuf.shape[0]
    copies = [
        pltpu.make_async_copy(src.at[b], dst.at[b], sem.at[i, b])
        for i, (src, dst) in enumerate([(kbuf, k_out), (vbuf, v_out)]) for b in range(rows)
    ]
    for copy in copies:
        copy.start()
    cols = 512

    def y_copy(c):
        span = pl.ds(pl.multiple_of(c * cols, cols), cols)
        return pltpu.make_async_copy(y_ref.at[:, span], y_out.at[:, span], y_sem.at[c])

    def project(c, carry):
        span = pl.ds(pl.multiple_of(c * cols, cols), cols)
        out = jnp.dot(att_ref[...], wo_ref[:, span], preferred_element_type=jnp.float32)
        y_ref[:, span] = (x_ref[:, span].astype(jnp.float32) + out).astype(jnp.bfloat16)
        y_copy(c).start()
        return carry

    lax.fori_loop(0, y_ref.shape[1] // cols, project, 0)
    for copy in copies:
        copy.wait()
    for c in range(y_ref.shape[1] // cols):
        y_copy(c).wait()


def solution(mesh):
    n = mesh.shape['cp']
    batch_spec = P(('dp', 'cp'))
    seq_spec = P('dp', 'cp')
    whole = P()
    hbm = pl.BlockSpec(memory_space=pl.ANY)
    vmem = pl.BlockSpec(memory_space=pltpu.VMEM)

    def per_device(x_tok, prompt_lens, k_cache, v_cache, norm_gain, w_q, b_q, w_k, b_k, w_v, b_v, w_o):
        rows, d_model = x_tok.shape
        batch, slots, kv_heads, head = k_cache.shape
        q_cols = w_q.shape[1]
        heads = q_cols // head
        q_rows = -(-heads // PACK) * PACK
        tiles = slots * kv_heads // PACK
        all_tiles = tiles * n
        block_rows = tiles * PACK
        cols = w_k.shape[1]
        half = head // 2
        freq = np.power(ROPE_THETA, -np.arange(half) * 2.0 / head).astype(np.float32)
        freq = jnp.asarray(np.concatenate([freq, freq])[None])
        parts = 4

        bf16, f32 = jnp.bfloat16, jnp.float32
        kbuf, vbuf, wo, att, x_near = pl.pallas_call(
            functools.partial(gather_kernel, n, kv_heads),
            out_shape=[
                pltpu.VMEM((rows, all_tiles, PACK, head), bf16),
                pltpu.VMEM((rows, all_tiles, PACK, head), bf16),
                pltpu.VMEM(w_o.shape, bf16),
                pltpu.VMEM((rows, q_cols), bf16),
                pltpu.VMEM((rows, d_model), bf16),
            ],
            in_specs=[hbm] * 13,
            out_specs=[vmem] * 5,
            scratch_shapes=[
                pltpu.SMEM((batch,), jnp.int32),
                pltpu.VMEM((1, head), f32),
                pltpu.VMEM((d_model,), bf16),
                pltpu.VMEM((q_cols,), bf16),
                pltpu.VMEM((cols,), bf16),
                pltpu.VMEM((cols,), bf16),
                pltpu.VMEM((3, d_model, cols), bf16),
                pltpu.VMEM((rows, d_model), bf16),
                pltpu.VMEM((rows, q_rows, head), f32),
                pltpu.VMEM((rows, PACK, head), f32),
                pltpu.VMEM((rows, PACK, head), f32),
                pltpu.VMEM((rows, n, q_rows, block_rows), f32),
                pltpu.VMEM((rows, n, q_rows, block_rows), bf16),
                pltpu.VMEM((rows, q_rows, head), f32),
                pltpu.VMEM((rows, q_rows, head), f32),
                pltpu.SemaphoreType.DMA((7,)),
                pltpu.SemaphoreType.DMA((3,)),
                pltpu.SemaphoreType.DMA,
                pltpu.SemaphoreType.DMA((n,)),
                pltpu.SemaphoreType.DMA((n,)),
                pltpu.SemaphoreType.DMA((n, parts)),
                pltpu.SemaphoreType.DMA((n, parts)),
            ],
            compiler_params=pltpu.CompilerParams(collective_id=0, has_side_effects=True, vmem_limit_bytes=28 * 1024 * 1024),
            name='gather_attend',
        )(prompt_lens, x_tok, freq, norm_gain, w_q, b_q, w_k, b_k, w_v, b_v, w_o,
          k_cache.reshape(batch, tiles, PACK, head), v_cache.reshape(batch, tiles, PACK, head))

        y_out, k_out, v_out = pl.pallas_call(
            finish_kernel,
            out_shape=[
                jax.ShapeDtypeStruct(x_tok.shape, bf16),
                jax.ShapeDtypeStruct(kbuf.shape, bf16),
                jax.ShapeDtypeStruct(vbuf.shape, bf16),
            ],
            in_specs=[vmem] * 5,
            out_specs=[hbm] * 3,
            scratch_shapes=[pltpu.VMEM(x_tok.shape, bf16), pltpu.SemaphoreType.DMA((2, rows)), pltpu.SemaphoreType.DMA((d_model // 512,))],
            compiler_params=pltpu.CompilerParams(vmem_limit_bytes=28 * 1024 * 1024),
            name='finish',
        )(*[pltpu.with_memory_space_constraint(a, pltpu.VMEM) for a in (kbuf, vbuf, wo, att, x_near)])
        shape = (rows, slots * n, kv_heads, head)
        return y_out, k_out.reshape(shape), v_out.reshape(shape)

    return jax.shard_map(per_device, mesh=mesh, in_specs=(batch_spec, P('dp'), seq_spec, seq_spec, whole, whole, whole, whole, whole, whole, whole, whole), out_specs=(batch_spec, batch_spec, batch_spec), check_vma=False)
```

```python
import functools

import jax
import jax.numpy as jnp
import numpy as np
from jax import lax
from jax.experimental import pallas as pl
from jax.experimental.pallas import tpu as pltpu
from jax.sharding import PartitionSpec as P

RMS_EPS = 1e-6
ROPE_THETA = 1000000.0
PACK = 16
LANES = 128
NEG = -1e30


def gather_kernel(n, kv_heads, lens_hbm, x_hbm, freq_hbm, gain_hbm, wq_hbm, bq_hbm, wk_hbm, bk_hbm, wv_hbm, bv_hbm, wo_hbm, k_hbm, v_hbm,
                  kbuf, vbuf, wo_ref, att_ref, x_ref,
                  lens, freq_ref, gain_ref, bq_ref, bk_ref, bv_ref, wbuf, h_ref, qf_ref, knew_ref, vnew_ref, s_ref, p_ref, acc_ref, sum_ref,
                  small_sem, wsem, wo_sem, k_send, k_recv, v_send, v_recv):
    rows, d_model = x_ref.shape
    head = acc_ref.shape[-1]
    q_rows = acc_ref.shape[1]
    heads = wq_hbm.shape[1] // head
    group = heads // kv_heads
    tiles = k_hbm.shape[1]
    block_rows = tiles * PACK
    slots = block_rows // kv_heads
    cols = wbuf.shape[2]
    me = lax.axis_index('cp')

    chip, core = me // 2, lax.rem(me, 2)
    chips = n // 2
    parts = v_recv.shape[1]
    part_rows = rows // parts

    fars = sorted(range(1, chips), key=lambda f: -min(f, chips - f))

    def place(t, way):
        far = sum(jnp.where(t // 2 == k + 1, f, 0) for k, f in enumerate(fars))
        return lax.rem(chip + way * far + chips, chips) * 2 + lax.rem(core + t, 2)

    def block(ref, owner, part, count):
        return ref.at[pl.ds(owner * rows + part * count, count)]

    def span(ref, sender, part, count):
        return ref.at[pl.ds(part * count, count), pl.ds(sender * tiles, tiles)]

    def keys_copy(to, sender):
        return pltpu.make_async_remote_copy(
            src_ref=block(k_hbm, to, 0, rows), dst_ref=span(kbuf, sender, 0, rows), send_sem=k_send.at[to], recv_sem=k_recv.at[sender],
            device_id={'cp': to}, device_id_type=pl.DeviceIdType.MESH)

    def values_copy(to, sender, part):
        return pltpu.make_async_remote_copy(
            src_ref=block(v_hbm, to, part, part_rows), dst_ref=span(vbuf, sender, part, part_rows), send_sem=v_send.at[to, part],
            recv_sem=v_recv.at[sender, part], device_id={'cp': to}, device_id_type=pl.DeviceIdType.MESH)

    barrier = pltpu.get_barrier_semaphore()
    for t in range(1, n):
        pl.semaphore_signal(barrier, inc=1, device_id={'cp': place(t, 1)}, device_id_type=pl.DeviceIdType.MESH)

    smalls = [
        pltpu.make_async_copy(src, dst, small_sem.at[i])
        for i, (src, dst) in enumerate([
            (lens_hbm, lens), (x_hbm, x_ref), (freq_hbm, freq_ref), (gain_hbm, gain_ref), (bq_hbm, bq_ref), (bk_hbm, bk_ref), (bv_hbm, bv_ref)])
    ]
    for copy in smalls:
        copy.start()

    blocks = [(wk_hbm, 0), (wv_hbm, 0)] + [(wq_hbm, c) for c in range(wq_hbm.shape[1] // cols)]

    def weight_copy(t):
        src, c = blocks[t]
        return pltpu.make_async_copy(src.at[:, pl.ds(c * cols, cols)], wbuf.at[t % wbuf.shape[0]], wsem.at[t % wbuf.shape[0]])

    for t in range(wbuf.shape[0]):
        weight_copy(t).start()

    pltpu.make_async_copy(block(k_hbm, me, 0, rows), span(kbuf, me, 0, rows), k_recv.at[me]).start()
    for part in range(parts):
        pltpu.make_async_copy(block(v_hbm, me, part, part_rows), span(vbuf, me, part, part_rows), v_recv.at[me, part]).start()

    pl.semaphore_wait(barrier, n - 1)
    for t in range(1, n):
        keys_copy(place(t, 1), me).start()
    for part in range(parts):
        for t in range(1, n):
            values_copy(place(t, 1), me, part).start()

    for copy in smalls:
        copy.wait()
    x_wide = x_ref[...].astype(jnp.float32)
    mean_sq = jnp.mean(x_wide * x_wide, axis=-1, keepdims=True)
    h_ref[...] = (x_wide * lax.rsqrt(mean_sq + RMS_EPS) * gain_ref[...].astype(jnp.float32)[None]).astype(jnp.bfloat16)
    row = lax.broadcasted_iota(jnp.int32, (rows, head), 0)
    lane = lax.broadcasted_iota(jnp.int32, (rows, head), 1)
    positions = sum(jnp.where(row == b, lens[me * rows + b], 0) for b in range(rows))
    angle = positions.astype(jnp.float32) * freq_ref[...]
    cos_t = jnp.cos(angle)
    sin_t = jnp.where(lane < head // 2, -jnp.sin(angle), jnp.sin(angle))

    def rotate(v):
        return v * cos_t + pltpu.roll(v, head // 2, 1) * sin_t

    qf_ref[...] = jnp.zeros_like(qf_ref)
    for t in range(len(blocks)):
        weight_copy(t).wait()
        out = jnp.dot(h_ref[...], wbuf[t % wbuf.shape[0]], preferred_element_type=jnp.float32)
        if t + wbuf.shape[0] < len(blocks):
            weight_copy(t + wbuf.shape[0]).start()
        c = blocks[t][1]
        bias = (bk_ref if t == 0 else bv_ref if t == 1 else bq_ref)[c * cols:(c + 1) * cols]
        out = out + bias.astype(jnp.float32)[None]
        for i in range(cols // head):
            part = out[:, i * head:(i + 1) * head]
            if t == 0:
                part = rotate(part).astype(jnp.bfloat16).astype(jnp.float32)
                for r in range(PACK // kv_heads):
                    knew_ref[:, r * kv_heads + i, :] = part
            elif t == 1:
                part = part.astype(jnp.bfloat16).astype(jnp.float32)
                for r in range(PACK // kv_heads):
                    vnew_ref[:, r * kv_heads + i, :] = part
            else:
                qf_ref[:, c * (cols // head) + i, :] = rotate(part)
    lane_width = wo_ref.shape[2]
    wo_copies = [pltpu.make_async_copy(wo_hbm.at[:, pl.ds(c * lane_width, lane_width)], wo_ref.at[c], wo_sem.at[c]) for c in range(wo_ref.shape[0])]
    for copy in wo_copies:
        copy.start()

    def merged(s, sender, buf, new_ref):
        pos = lens[me * rows + s]
        tile = buf[s, pl.ds(sender * tiles, tiles)].astype(jnp.float32)
        shape = (tiles, PACK, head)
        slot = sender * slots + lax.broadcasted_iota(jnp.int32, shape, 0) * (PACK // kv_heads) + lax.broadcasted_iota(jnp.int32, shape, 1) // kv_heads
        new = jnp.broadcast_to(new_ref[s][None], shape)
        tile = jnp.where(slot < pos, tile, jnp.where(slot == pos, new, 0.0)).astype(jnp.bfloat16)
        buf[s, pl.ds(sender * tiles, tiles)] = tile
        return tile.reshape(block_rows, head)

    def keys_step(s, sender):
        pos = lens[me * rows + s]
        keys = merged(s, sender, kbuf, knew_ref)
        query = qf_ref[s].astype(jnp.bfloat16)
        scores = lax.dot_general(query, keys, (((1,), (1,)), ((), ())), preferred_element_type=jnp.float32) * (head ** -0.5)
        row = lax.broadcasted_iota(jnp.int32, scores.shape, 0)
        col = lax.broadcasted_iota(jnp.int32, scores.shape, 1)
        valid = (col % kv_heads == row // group) & (sender * slots + col // kv_heads <= pos)
        s_ref[s, sender] = jnp.where(valid, scores, NEG)
        return 0

    def soften(s):
        scores = s_ref[s]
        top = jnp.max(jnp.max(scores, axis=0), axis=-1, keepdims=True)
        weights = jnp.exp(scores - top[None])
        sum_ref[s] = jnp.broadcast_to(jnp.sum(jnp.sum(weights, axis=0), axis=-1, keepdims=True), (q_rows, head))
        p_ref[s] = weights.astype(jnp.bfloat16)
        return 0

    def values_step(s, sender):
        values = merged(s, sender, vbuf, vnew_ref)
        acc_ref[s] += jnp.dot(p_ref[s, sender], values, preferred_element_type=jnp.float32)
        return 0

    def attended_row(s):
        att_ref[s] = acc_ref[s] / sum_ref[s]
        return 0

    def keys_arrival(t, carry):
        sender = place(t, -1)
        keys_copy(sender, sender).wait_recv()
        return lax.fori_loop(0, rows, lambda s, c: keys_step(s, sender), carry)

    def values_arrival(u, carry):
        part, sender = u // n, place(lax.rem(u, n), -1)
        values_copy(sender, sender, part).wait_recv()
        lax.fori_loop(part * part_rows, (part + 1) * part_rows, lambda s, c: values_step(s, sender), carry)

        @pl.when(lax.rem(u, n) == n - 1)
        def _():
            lax.fori_loop(part * part_rows, (part + 1) * part_rows, lambda s, c: attended_row(s), carry)

        return carry

    lax.fori_loop(0, n, keys_arrival, 0)
    lax.fori_loop(0, rows, lambda s, c: soften(s), 0)
    acc_ref[...] = jnp.zeros_like(acc_ref)
    for copy in wo_copies:
        copy.wait()
    lax.fori_loop(0, n * parts, values_arrival, 0)

    for t in range(1, n):
        keys_copy(place(t, 1), me).wait_send()
        for part in range(parts):
            values_copy(place(t, 1), me, part).wait_send()


def finish_kernel(kbuf, vbuf, wo_ref, att_ref, x_ref, y_out, k_out, v_out, y_ref, sem, y_sem):
    rows = kbuf.shape[0]
    copies = [
        pltpu.make_async_copy(src.at[b], dst.at[b], sem.at[i, b])
        for i, (src, dst) in enumerate([(kbuf, k_out), (vbuf, v_out)]) for b in range(rows)
    ]
    for copy in copies:
        copy.start()
    strips = 4
    cols = strips * LANES
    heads = wo_ref.shape[1] // att_ref.shape[2]
    attended = jnp.concatenate([att_ref[:, j, :] for j in range(heads)], axis=1).astype(jnp.bfloat16)

    def project(c, carry):
        span = pl.ds(pl.multiple_of(c * cols, cols), cols)
        weights = jnp.concatenate([wo_ref[c * strips + i] for i in range(strips)], axis=1)
        out = jnp.dot(attended, weights, preferred_element_type=jnp.float32)
        y_ref[:, span] = (x_ref[:, span].astype(jnp.float32) + out).astype(jnp.bfloat16)
        return carry

    lax.fori_loop(0, y_ref.shape[1] // cols, project, 0)
    y_copy = pltpu.make_async_copy(y_ref, y_out, y_sem)
    y_copy.start()
    for copy in copies:
        copy.wait()
    y_copy.wait()


def solution(mesh):
    n = mesh.shape['cp']
    batch_spec = P(('dp', 'cp'))
    seq_spec = P('dp', 'cp')
    whole = P()
    hbm = pl.BlockSpec(memory_space=pl.ANY)
    vmem = pl.BlockSpec(memory_space=pltpu.VMEM)

    def per_device(x_tok, prompt_lens, k_cache, v_cache, norm_gain, w_q, b_q, w_k, b_k, w_v, b_v, w_o):
        rows, d_model = x_tok.shape
        batch, slots, kv_heads, head = k_cache.shape
        q_cols = w_q.shape[1]
        heads = q_cols // head
        q_rows = -(-heads // PACK) * PACK
        tiles = slots * kv_heads // PACK
        all_tiles = tiles * n
        block_rows = tiles * PACK
        cols = w_k.shape[1]
        half = head // 2
        freq = np.power(ROPE_THETA, -np.arange(half) * 2.0 / head).astype(np.float32)
        freq = jnp.asarray(np.concatenate([freq, freq])[None])
        parts = 4

        bf16, f32 = jnp.bfloat16, jnp.float32
        kbuf, vbuf, wo, att, x_near = pl.pallas_call(
            functools.partial(gather_kernel, n, kv_heads),
            out_shape=[
                pltpu.VMEM((rows, all_tiles, PACK, head), bf16),
                pltpu.VMEM((rows, all_tiles, PACK, head), bf16),
                pltpu.VMEM((w_o.shape[1] // LANES, w_o.shape[0], LANES), bf16),
                pltpu.VMEM((rows, q_rows, head), f32),
                pltpu.VMEM((rows, d_model), bf16),
            ],
            in_specs=[hbm] * 13,
            out_specs=[vmem] * 5,
            scratch_shapes=[
                pltpu.SMEM((batch,), jnp.int32),
                pltpu.VMEM((1, head), f32),
                pltpu.VMEM((d_model,), bf16),
                pltpu.VMEM((q_cols,), bf16),
                pltpu.VMEM((cols,), bf16),
                pltpu.VMEM((cols,), bf16),
                pltpu.VMEM((3, d_model, cols), bf16),
                pltpu.VMEM((rows, d_model), bf16),
                pltpu.VMEM((rows, q_rows, head), f32),
                pltpu.VMEM((rows, PACK, head), f32),
                pltpu.VMEM((rows, PACK, head), f32),
                pltpu.VMEM((rows, n, q_rows, block_rows), f32),
                pltpu.VMEM((rows, n, q_rows, block_rows), bf16),
                pltpu.VMEM((rows, q_rows, head), f32),
                pltpu.VMEM((rows, q_rows, head), f32),
                pltpu.SemaphoreType.DMA((7,)),
                pltpu.SemaphoreType.DMA((3,)),
                pltpu.SemaphoreType.DMA((w_o.shape[1] // LANES,)),
                pltpu.SemaphoreType.DMA((n,)),
                pltpu.SemaphoreType.DMA((n,)),
                pltpu.SemaphoreType.DMA((n, parts)),
                pltpu.SemaphoreType.DMA((n, parts)),
            ],
            compiler_params=pltpu.CompilerParams(collective_id=0, has_side_effects=True, vmem_limit_bytes=28 * 1024 * 1024),
            name='gather_attend',
        )(prompt_lens, x_tok, freq, norm_gain, w_q, b_q, w_k, b_k, w_v, b_v, w_o,
          k_cache.reshape(batch, tiles, PACK, head), v_cache.reshape(batch, tiles, PACK, head))

        y_out, k_out, v_out = pl.pallas_call(
            finish_kernel,
            out_shape=[
                jax.ShapeDtypeStruct(x_tok.shape, bf16),
                jax.ShapeDtypeStruct(kbuf.shape, bf16),
                jax.ShapeDtypeStruct(vbuf.shape, bf16),
            ],
            in_specs=[vmem] * 5,
            out_specs=[hbm] * 3,
            scratch_shapes=[pltpu.VMEM(x_tok.shape, bf16), pltpu.SemaphoreType.DMA((2, rows)), pltpu.SemaphoreType.DMA],
            compiler_params=pltpu.CompilerParams(vmem_limit_bytes=28 * 1024 * 1024),
            name='finish',
        )(*[pltpu.with_memory_space_constraint(a, pltpu.VMEM) for a in (kbuf, vbuf, wo, att, x_near)])
        shape = (rows, slots * n, kv_heads, head)
        return y_out, k_out.reshape(shape), v_out.reshape(shape)

    return jax.shard_map(per_device, mesh=mesh, in_specs=(batch_spec, P('dp'), seq_spec, seq_spec, whole, whole, whole, whole, whole, whole, whole, whole), out_specs=(batch_spec, batch_spec, batch_spec), check_vma=False)
```

```python
import functools

import jax
import jax.numpy as jnp
import numpy as np
from jax import lax
from jax.experimental import pallas as pl
from jax.experimental.pallas import tpu as pltpu
from jax.sharding import PartitionSpec as P

RMS_EPS = 1e-6
ROPE_THETA = 1000000.0
PACK = 16
LANES = 128
NEG = -1e30


def gather_kernel(n, kv_heads, lens_hbm, x_hbm, freq_hbm, gain_hbm, wq_hbm, bq_hbm, wk_hbm, bk_hbm, wv_hbm, bv_hbm, wo_hbm, k_hbm, v_hbm,
                  kbuf, vbuf, wo_ref, att_ref, x_ref,
                  lens, freq_ref, gain_ref, bq_ref, bk_ref, bv_ref, wbuf, h_ref, qf_ref, knew_ref, vnew_ref, s_ref, p_ref, acc_ref, sum_ref,
                  small_sem, wsem, wo_sem, k_send, k_recv, v_send, v_recv, far_sem):
    rows, d_model = x_ref.shape
    head = acc_ref.shape[-1]
    q_rows = acc_ref.shape[1]
    heads = wq_hbm.shape[1] // head
    group = heads // kv_heads
    tiles = k_hbm.shape[1]
    block_rows = tiles * PACK
    slots = block_rows // kv_heads
    cols = wbuf.shape[2]
    me = lax.axis_index('cp')

    chip, core = me // 2, lax.rem(me, 2)
    chips = n // 2
    parts = v_recv.shape[1]
    part_rows = rows // parts

    fars = sorted(range(1, chips), key=lambda f: min(f, chips - f))
    near = 2 * sum(min(f, chips - f) == 1 for f in fars) + 2
    assert chips == 4 and near == 6

    def place(t, way):
        far = sum(jnp.where(t // 2 == k + 1, f, 0) for k, f in enumerate(fars))
        return lax.rem(chip + way * far + chips, chips) * 2 + lax.rem(core + t, 2)

    def block(ref, owner, part, count):
        return ref.at[pl.ds(owner * rows + part * count, count)]

    def span(ref, sender, part, count):
        return ref.at[pl.ds(part * count, count), pl.ds(sender * tiles, tiles)]

    def keys_copy(to, sender):
        return pltpu.make_async_remote_copy(
            src_ref=block(k_hbm, to, 0, rows), dst_ref=span(kbuf, sender, 0, rows), send_sem=k_send.at[to], recv_sem=k_recv.at[sender],
            device_id={'cp': to}, device_id_type=pl.DeviceIdType.MESH)

    def values_copy(to, sender, part):
        return pltpu.make_async_remote_copy(
            src_ref=block(v_hbm, to, part, part_rows), dst_ref=span(vbuf, sender, part, part_rows), send_sem=v_send.at[to, part],
            recv_sem=v_recv.at[sender, part], device_id={'cp': to}, device_id_type=pl.DeviceIdType.MESH)

    barrier = pltpu.get_barrier_semaphore()
    for t in range(1, near):
        pl.semaphore_signal(barrier, inc=1, device_id={'cp': place(t, 1)}, device_id_type=pl.DeviceIdType.MESH)

    smalls = [
        pltpu.make_async_copy(src, dst, small_sem.at[i])
        for i, (src, dst) in enumerate([
            (lens_hbm, lens), (x_hbm, x_ref), (freq_hbm, freq_ref), (gain_hbm, gain_ref), (bq_hbm, bq_ref), (bk_hbm, bk_ref), (bv_hbm, bv_ref)])
    ]
    for copy in smalls:
        copy.start()

    blocks = [(wk_hbm, 0), (wv_hbm, 0)] + [(wq_hbm, c) for c in range(wq_hbm.shape[1] // cols)]

    def weight_copy(t):
        src, c = blocks[t]
        return pltpu.make_async_copy(src.at[:, pl.ds(c * cols, cols)], wbuf.at[t % wbuf.shape[0]], wsem.at[t % wbuf.shape[0]])

    for t in range(wbuf.shape[0]):
        weight_copy(t).start()

    pltpu.make_async_copy(block(k_hbm, me, 0, rows), span(kbuf, me, 0, rows), k_recv.at[me]).start()
    for part in range(parts):
        pltpu.make_async_copy(block(v_hbm, me, part, part_rows), span(vbuf, me, part, part_rows), v_recv.at[me, part]).start()

    pl.semaphore_wait(barrier, near - 1)
    for t in range(1, near):
        keys_copy(place(t, 1), me).start()
    for t in range(2, near, 2):
        pl.semaphore_signal(far_sem, inc=1, device_id={'cp': place(t, 1)}, device_id_type=pl.DeviceIdType.MESH)
    pl.semaphore_wait(far_sem, near // 2 - 1)
    for t in range(near, n):
        keys_copy(place(t, 1), me).start()
    for part in range(parts):
        for t in range(1, n):
            values_copy(place(t, 1), me, part).start()

    for copy in smalls:
        copy.wait()
    x_wide = x_ref[...].astype(jnp.float32)
    mean_sq = jnp.mean(x_wide * x_wide, axis=-1, keepdims=True)
    h_ref[...] = (x_wide * lax.rsqrt(mean_sq + RMS_EPS) * gain_ref[...].astype(jnp.float32)[None]).astype(jnp.bfloat16)
    row = lax.broadcasted_iota(jnp.int32, (rows, head), 0)
    lane = lax.broadcasted_iota(jnp.int32, (rows, head), 1)
    positions = sum(jnp.where(row == b, lens[me * rows + b], 0) for b in range(rows))
    angle = positions.astype(jnp.float32) * freq_ref[...]
    cos_t = jnp.cos(angle)
    sin_t = jnp.where(lane < head // 2, -jnp.sin(angle), jnp.sin(angle))

    def rotate(v):
        return v * cos_t + pltpu.roll(v, head // 2, 1) * sin_t

    qf_ref[...] = jnp.zeros_like(qf_ref)
    for t in range(len(blocks)):
        weight_copy(t).wait()
        out = jnp.dot(h_ref[...], wbuf[t % wbuf.shape[0]], preferred_element_type=jnp.float32)
        if t + wbuf.shape[0] < len(blocks):
            weight_copy(t + wbuf.shape[0]).start()
        c = blocks[t][1]
        bias = (bk_ref if t == 0 else bv_ref if t == 1 else bq_ref)[c * cols:(c + 1) * cols]
        out = out + bias.astype(jnp.float32)[None]
        for i in range(cols // head):
            part = out[:, i * head:(i + 1) * head]
            if t == 0:
                part = rotate(part).astype(jnp.bfloat16).astype(jnp.float32)
                for r in range(PACK // kv_heads):
                    knew_ref[:, r * kv_heads + i, :] = part
            elif t == 1:
                part = part.astype(jnp.bfloat16).astype(jnp.float32)
                for r in range(PACK // kv_heads):
                    vnew_ref[:, r * kv_heads + i, :] = part
            else:
                qf_ref[:, c * (cols // head) + i, :] = rotate(part)
    lane_width = wo_ref.shape[2]
    wo_copies = [pltpu.make_async_copy(wo_hbm.at[:, pl.ds(c * lane_width, lane_width)], wo_ref.at[c], wo_sem.at[c]) for c in range(wo_ref.shape[0])]
    for copy in wo_copies:
        copy.start()

    def merged(s, sender, buf, new_ref):
        pos = lens[me * rows + s]
        tile = buf[s, pl.ds(sender * tiles, tiles)].astype(jnp.float32)
        shape = (tiles, PACK, head)
        slot = sender * slots + lax.broadcasted_iota(jnp.int32, shape, 0) * (PACK // kv_heads) + lax.broadcasted_iota(jnp.int32, shape, 1) // kv_heads
        new = jnp.broadcast_to(new_ref[s][None], shape)
        tile = jnp.where(slot < pos, tile, jnp.where(slot == pos, new, 0.0)).astype(jnp.bfloat16)
        buf[s, pl.ds(sender * tiles, tiles)] = tile
        return tile.reshape(block_rows, head)

    def keys_step(s, sender):
        pos = lens[me * rows + s]
        keys = merged(s, sender, kbuf, knew_ref)
        query = qf_ref[s].astype(jnp.bfloat16)
        scores = lax.dot_general(query, keys, (((1,), (1,)), ((), ())), preferred_element_type=jnp.float32) * (head ** -0.5)
        row = lax.broadcasted_iota(jnp.int32, scores.shape, 0)
        col = lax.broadcasted_iota(jnp.int32, scores.shape, 1)
        valid = (col % kv_heads == row // group) & (sender * slots + col // kv_heads <= pos)
        s_ref[s, sender] = jnp.where(valid, scores, NEG)
        return 0

    def soften(s):
        scores = s_ref[s]
        top = jnp.max(jnp.max(scores, axis=0), axis=-1, keepdims=True)
        weights = jnp.exp(scores - top[None])
        sum_ref[s] = jnp.broadcast_to(jnp.sum(jnp.sum(weights, axis=0), axis=-1, keepdims=True), (q_rows, head))
        p_ref[s] = weights.astype(jnp.bfloat16)
        return 0

    def values_step(s, sender):
        values = merged(s, sender, vbuf, vnew_ref)
        acc_ref[s] += jnp.dot(p_ref[s, sender], values, preferred_element_type=jnp.float32)
        return 0

    def attended_row(s):
        att_ref[s] = acc_ref[s] / sum_ref[s]
        return 0

    def keys_arrival(t, carry):
        sender = place(t, -1)
        keys_copy(sender, sender).wait_recv()
        return lax.fori_loop(0, rows, lambda s, c: keys_step(s, sender), carry)

    def values_arrival(u, carry):
        part, sender = u // n, place(lax.rem(u, n), -1)
        values_copy(sender, sender, part).wait_recv()
        lax.fori_loop(part * part_rows, (part + 1) * part_rows, lambda s, c: values_step(s, sender), carry)

        @pl.when(lax.rem(u, n) == n - 1)
        def _():
            lax.fori_loop(part * part_rows, (part + 1) * part_rows, lambda s, c: attended_row(s), carry)

        return carry

    lax.fori_loop(0, n, keys_arrival, 0)
    lax.fori_loop(0, rows, lambda s, c: soften(s), 0)
    acc_ref[...] = jnp.zeros_like(acc_ref)
    for copy in wo_copies:
        copy.wait()
    lax.fori_loop(0, n * parts, values_arrival, 0)

    for t in range(1, n):
        keys_copy(place(t, 1), me).wait_send()
        for part in range(parts):
            values_copy(place(t, 1), me, part).wait_send()


def finish_kernel(kbuf, vbuf, wo_ref, att_ref, x_ref, y_out, k_out, v_out, y_ref, sem, y_sem):
    rows = kbuf.shape[0]
    copies = [
        pltpu.make_async_copy(src.at[b], dst.at[b], sem.at[i, b])
        for i, (src, dst) in enumerate([(kbuf, k_out), (vbuf, v_out)]) for b in range(rows)
    ]
    for copy in copies:
        copy.start()
    strips = 4
    cols = strips * LANES
    heads = wo_ref.shape[1] // att_ref.shape[2]
    attended = jnp.concatenate([att_ref[:, j, :] for j in range(heads)], axis=1).astype(jnp.bfloat16)

    def project(c, carry):
        span = pl.ds(pl.multiple_of(c * cols, cols), cols)
        weights = jnp.concatenate([wo_ref[c * strips + i] for i in range(strips)], axis=1)
        out = jnp.dot(attended, weights, preferred_element_type=jnp.float32)
        y_ref[:, span] = (x_ref[:, span].astype(jnp.float32) + out).astype(jnp.bfloat16)
        return carry

    lax.fori_loop(0, y_ref.shape[1] // cols, project, 0)
    y_copy = pltpu.make_async_copy(y_ref, y_out, y_sem)
    y_copy.start()
    for copy in copies:
        copy.wait()
    y_copy.wait()


def solution(mesh):
    n = mesh.shape['cp']
    batch_spec = P(('dp', 'cp'))
    seq_spec = P('dp', 'cp')
    whole = P()
    hbm = pl.BlockSpec(memory_space=pl.ANY)
    vmem = pl.BlockSpec(memory_space=pltpu.VMEM)

    def per_device(x_tok, prompt_lens, k_cache, v_cache, norm_gain, w_q, b_q, w_k, b_k, w_v, b_v, w_o):
        rows, d_model = x_tok.shape
        batch, slots, kv_heads, head = k_cache.shape
        q_cols = w_q.shape[1]
        heads = q_cols // head
        q_rows = -(-heads // PACK) * PACK
        tiles = slots * kv_heads // PACK
        all_tiles = tiles * n
        block_rows = tiles * PACK
        cols = w_k.shape[1]
        half = head // 2
        freq = np.power(ROPE_THETA, -np.arange(half) * 2.0 / head).astype(np.float32)
        freq = jnp.asarray(np.concatenate([freq, freq])[None])
        parts = 4

        bf16, f32 = jnp.bfloat16, jnp.float32
        kbuf, vbuf, wo, att, x_near = pl.pallas_call(
            functools.partial(gather_kernel, n, kv_heads),
            out_shape=[
                pltpu.VMEM((rows, all_tiles, PACK, head), bf16),
                pltpu.VMEM((rows, all_tiles, PACK, head), bf16),
                pltpu.VMEM((w_o.shape[1] // LANES, w_o.shape[0], LANES), bf16),
                pltpu.VMEM((rows, q_rows, head), f32),
                pltpu.VMEM((rows, d_model), bf16),
            ],
            in_specs=[hbm] * 13,
            out_specs=[vmem] * 5,
            scratch_shapes=[
                pltpu.SMEM((batch,), jnp.int32),
                pltpu.VMEM((1, head), f32),
                pltpu.VMEM((d_model,), bf16),
                pltpu.VMEM((q_cols,), bf16),
                pltpu.VMEM((cols,), bf16),
                pltpu.VMEM((cols,), bf16),
                pltpu.VMEM((3, d_model, cols), bf16),
                pltpu.VMEM((rows, d_model), bf16),
                pltpu.VMEM((rows, q_rows, head), f32),
                pltpu.VMEM((rows, PACK, head), f32),
                pltpu.VMEM((rows, PACK, head), f32),
                pltpu.VMEM((rows, n, q_rows, block_rows), f32),
                pltpu.VMEM((rows, n, q_rows, block_rows), bf16),
                pltpu.VMEM((rows, q_rows, head), f32),
                pltpu.VMEM((rows, q_rows, head), f32),
                pltpu.SemaphoreType.DMA((7,)),
                pltpu.SemaphoreType.DMA((3,)),
                pltpu.SemaphoreType.DMA((w_o.shape[1] // LANES,)),
                pltpu.SemaphoreType.DMA((n,)),
                pltpu.SemaphoreType.DMA((n,)),
                pltpu.SemaphoreType.DMA((n, parts)),
                pltpu.SemaphoreType.DMA((n, parts)),
                pltpu.SemaphoreType.REGULAR,
            ],
            compiler_params=pltpu.CompilerParams(collective_id=0, has_side_effects=True, vmem_limit_bytes=28 * 1024 * 1024),
            name='gather_attend',
        )(prompt_lens, x_tok, freq, norm_gain, w_q, b_q, w_k, b_k, w_v, b_v, w_o,
          k_cache.reshape(batch, tiles, PACK, head), v_cache.reshape(batch, tiles, PACK, head))

        y_out, k_out, v_out = pl.pallas_call(
            finish_kernel,
            out_shape=[
                jax.ShapeDtypeStruct(x_tok.shape, bf16),
                jax.ShapeDtypeStruct(kbuf.shape, bf16),
                jax.ShapeDtypeStruct(vbuf.shape, bf16),
            ],
            in_specs=[vmem] * 5,
            out_specs=[hbm] * 3,
            scratch_shapes=[pltpu.VMEM(x_tok.shape, bf16), pltpu.SemaphoreType.DMA((2, rows)), pltpu.SemaphoreType.DMA],
            compiler_params=pltpu.CompilerParams(vmem_limit_bytes=28 * 1024 * 1024),
            name='finish',
        )(*[pltpu.with_memory_space_constraint(a, pltpu.VMEM) for a in (kbuf, vbuf, wo, att, x_near)])
        shape = (rows, slots * n, kv_heads, head)
        return y_out, k_out.reshape(shape), v_out.reshape(shape)

    return jax.shard_map(per_device, mesh=mesh, in_specs=(batch_spec, P('dp'), seq_spec, seq_spec, whole, whole, whole, whole, whole, whole, whole, whole), out_specs=(batch_spec, batch_spec, batch_spec), check_vma=False)
```

```python
import functools

import jax
import jax.numpy as jnp
import numpy as np
from jax import lax
from jax.experimental import pallas as pl
from jax.experimental.pallas import tpu as pltpu
from jax.sharding import PartitionSpec as P

RMS_EPS = 1e-6
ROPE_THETA = 1000000.0
PACK = 16
LANES = 128
NEG = -1e30


def gather_kernel(n, kv_heads, lens_hbm, x_hbm, freq_hbm, gain_hbm, wq_hbm, bq_hbm, wk_hbm, bk_hbm, wv_hbm, bv_hbm, wo_hbm, k_hbm, v_hbm,
                  kbuf, vbuf, wo_ref, att_ref, x_ref,
                  lens, freq_ref, gain_ref, bq_ref, bk_ref, bv_ref, wbuf, h_ref, qf_ref, knew_ref, vnew_ref, s_ref, p_ref, acc_ref, sum_ref,
                  small_sem, wsem, wo_sem, k_send, k_recv, v_send, v_recv, far_sem):
    rows, d_model = x_ref.shape
    head = acc_ref.shape[-1]
    q_rows = acc_ref.shape[1]
    heads = wq_hbm.shape[1] // head
    group = heads // kv_heads
    tiles = k_hbm.shape[1]
    block_rows = tiles * PACK
    slots = block_rows // kv_heads
    cols = wbuf.shape[2]
    me = lax.axis_index('cp')

    chip, core = me // 2, lax.rem(me, 2)
    chips = n // 2
    parts = v_recv.shape[1]
    part_rows = rows // parts

    fars = sorted(range(1, chips), key=lambda f: min(f, chips - f))
    near = 2 * sum(min(f, chips - f) == 1 for f in fars) + 2
    assert chips == 4 and near == 6

    def place(t, way):
        far = sum(jnp.where(t // 2 == k + 1, f, 0) for k, f in enumerate(fars))
        return lax.rem(chip + way * far + chips, chips) * 2 + lax.rem(core + t, 2)

    values_order = [*range(near, n), *range(1, near)]

    def block(ref, owner, part, count):
        return ref.at[pl.ds(owner * rows + part * count, count)]

    def span(ref, sender, part, count):
        return ref.at[pl.ds(part * count, count), pl.ds(sender * tiles, tiles)]

    def keys_copy(to, sender):
        return pltpu.make_async_remote_copy(
            src_ref=block(k_hbm, to, 0, rows), dst_ref=span(kbuf, sender, 0, rows), send_sem=k_send.at[to], recv_sem=k_recv.at[sender],
            device_id={'cp': to}, device_id_type=pl.DeviceIdType.MESH)

    def values_copy(to, sender, part):
        return pltpu.make_async_remote_copy(
            src_ref=block(v_hbm, to, part, part_rows), dst_ref=span(vbuf, sender, part, part_rows), send_sem=v_send.at[to, part],
            recv_sem=v_recv.at[sender, part], device_id={'cp': to}, device_id_type=pl.DeviceIdType.MESH)

    barrier = pltpu.get_barrier_semaphore()
    for t in range(1, near):
        pl.semaphore_signal(barrier, inc=1, device_id={'cp': place(t, 1)}, device_id_type=pl.DeviceIdType.MESH)

    smalls = [
        pltpu.make_async_copy(src, dst, small_sem.at[i])
        for i, (src, dst) in enumerate([
            (lens_hbm, lens), (x_hbm, x_ref), (freq_hbm, freq_ref), (gain_hbm, gain_ref), (bq_hbm, bq_ref), (bk_hbm, bk_ref), (bv_hbm, bv_ref)])
    ]
    for copy in smalls:
        copy.start()

    blocks = [(wk_hbm, 0), (wv_hbm, 0)] + [(wq_hbm, c) for c in range(wq_hbm.shape[1] // cols)]

    def weight_copy(t):
        src, c = blocks[t]
        return pltpu.make_async_copy(src.at[:, pl.ds(c * cols, cols)], wbuf.at[t % wbuf.shape[0]], wsem.at[t % wbuf.shape[0]])

    for t in range(wbuf.shape[0]):
        weight_copy(t).start()

    pltpu.make_async_copy(block(k_hbm, me, 0, rows), span(kbuf, me, 0, rows), k_recv.at[me]).start()
    for part in range(parts):
        pltpu.make_async_copy(block(v_hbm, me, part, part_rows), span(vbuf, me, part, part_rows), v_recv.at[me, part]).start()

    pl.semaphore_wait(barrier, near - 1)
    for t in range(1, near):
        keys_copy(place(t, 1), me).start()
    for t in range(2, near, 2):
        pl.semaphore_signal(far_sem, inc=1, device_id={'cp': place(t, 1)}, device_id_type=pl.DeviceIdType.MESH)
    pl.semaphore_wait(far_sem, near // 2 - 1)
    for t in range(near, n):
        keys_copy(place(t, 1), me).start()
    for part in range(parts):
        for t in values_order:
            values_copy(place(t, 1), me, part).start()

    for copy in smalls:
        copy.wait()
    x_wide = x_ref[...].astype(jnp.float32)
    mean_sq = jnp.mean(x_wide * x_wide, axis=-1, keepdims=True)
    h_ref[...] = (x_wide * lax.rsqrt(mean_sq + RMS_EPS) * gain_ref[...].astype(jnp.float32)[None]).astype(jnp.bfloat16)
    row = lax.broadcasted_iota(jnp.int32, (rows, head), 0)
    lane = lax.broadcasted_iota(jnp.int32, (rows, head), 1)
    positions = sum(jnp.where(row == b, lens[me * rows + b], 0) for b in range(rows))
    angle = positions.astype(jnp.float32) * freq_ref[...]
    cos_t = jnp.cos(angle)
    sin_t = jnp.where(lane < head // 2, -jnp.sin(angle), jnp.sin(angle))

    def rotate(v):
        return v * cos_t + pltpu.roll(v, head // 2, 1) * sin_t

    qf_ref[...] = jnp.zeros_like(qf_ref)
    for t in range(len(blocks)):
        weight_copy(t).wait()
        out = jnp.dot(h_ref[...], wbuf[t % wbuf.shape[0]], preferred_element_type=jnp.float32)
        if t + wbuf.shape[0] < len(blocks):
            weight_copy(t + wbuf.shape[0]).start()
        c = blocks[t][1]
        bias = (bk_ref if t == 0 else bv_ref if t == 1 else bq_ref)[c * cols:(c + 1) * cols]
        out = out + bias.astype(jnp.float32)[None]
        for i in range(cols // head):
            part = out[:, i * head:(i + 1) * head]
            if t == 0:
                part = rotate(part).astype(jnp.bfloat16).astype(jnp.float32)
                for r in range(PACK // kv_heads):
                    knew_ref[:, r * kv_heads + i, :] = part
            elif t == 1:
                part = part.astype(jnp.bfloat16).astype(jnp.float32)
                for r in range(PACK // kv_heads):
                    vnew_ref[:, r * kv_heads + i, :] = part
            else:
                qf_ref[:, c * (cols // head) + i, :] = rotate(part)
    lane_width = wo_ref.shape[2]
    wo_copies = [pltpu.make_async_copy(wo_hbm.at[:, pl.ds(c * lane_width, lane_width)], wo_ref.at[c], wo_sem.at[c]) for c in range(wo_ref.shape[0])]
    for copy in wo_copies:
        copy.start()

    def merged(s, sender, buf, new_ref):
        pos = lens[me * rows + s]
        tile = buf[s, pl.ds(sender * tiles, tiles)].astype(jnp.float32)
        shape = (tiles, PACK, head)
        slot = sender * slots + lax.broadcasted_iota(jnp.int32, shape, 0) * (PACK // kv_heads) + lax.broadcasted_iota(jnp.int32, shape, 1) // kv_heads
        new = jnp.broadcast_to(new_ref[s][None], shape)
        tile = jnp.where(slot < pos, tile, jnp.where(slot == pos, new, 0.0)).astype(jnp.bfloat16)
        buf[s, pl.ds(sender * tiles, tiles)] = tile
        return tile.reshape(block_rows, head)

    def keys_step(s, sender):
        pos = lens[me * rows + s]
        keys = merged(s, sender, kbuf, knew_ref)
        query = qf_ref[s].astype(jnp.bfloat16)
        scores = lax.dot_general(query, keys, (((1,), (1,)), ((), ())), preferred_element_type=jnp.float32) * (head ** -0.5)
        row = lax.broadcasted_iota(jnp.int32, scores.shape, 0)
        col = lax.broadcasted_iota(jnp.int32, scores.shape, 1)
        valid = (col % kv_heads == row // group) & (sender * slots + col // kv_heads <= pos)
        s_ref[s, sender] = jnp.where(valid, scores, NEG)
        return 0

    def soften(s):
        scores = s_ref[s]
        top = jnp.max(jnp.max(scores, axis=0), axis=-1, keepdims=True)
        weights = jnp.exp(scores - top[None])
        sum_ref[s] = jnp.broadcast_to(jnp.sum(jnp.sum(weights, axis=0), axis=-1, keepdims=True), (q_rows, head))
        p_ref[s] = weights.astype(jnp.bfloat16)
        return 0

    def values_step(s, sender):
        values = merged(s, sender, vbuf, vnew_ref)
        acc_ref[s] += jnp.dot(p_ref[s, sender], values, preferred_element_type=jnp.float32)
        return 0

    def attended_row(s):
        att_ref[s] = acc_ref[s] / sum_ref[s]
        return 0

    def keys_arrival(t, carry):
        sender = place(t, -1)
        keys_copy(sender, sender).wait_recv()
        return lax.fori_loop(0, rows, lambda s, c: keys_step(s, sender), carry)

    def values_arrival(u, carry):
        part, sender = u // n, place(lax.rem(lax.rem(u, n) + near, n), -1)
        values_copy(sender, sender, part).wait_recv()
        lax.fori_loop(part * part_rows, (part + 1) * part_rows, lambda s, c: values_step(s, sender), carry)

        @pl.when(lax.rem(u, n) == n - 1)
        def _():
            lax.fori_loop(part * part_rows, (part + 1) * part_rows, lambda s, c: attended_row(s), carry)

        return carry

    lax.fori_loop(0, n, keys_arrival, 0)
    lax.fori_loop(0, rows, lambda s, c: soften(s), 0)
    acc_ref[...] = jnp.zeros_like(acc_ref)
    for copy in wo_copies:
        copy.wait()
    lax.fori_loop(0, n * parts, values_arrival, 0)

    for t in range(1, n):
        keys_copy(place(t, 1), me).wait_send()
        for part in range(parts):
            values_copy(place(t, 1), me, part).wait_send()


def finish_kernel(kbuf, vbuf, wo_ref, att_ref, x_ref, y_out, k_out, v_out, y_ref, sem, y_sem):
    rows = kbuf.shape[0]
    copies = [
        pltpu.make_async_copy(src.at[b], dst.at[b], sem.at[i, b])
        for i, (src, dst) in enumerate([(kbuf, k_out), (vbuf, v_out)]) for b in range(rows)
    ]
    for copy in copies:
        copy.start()
    strips = 4
    cols = strips * LANES
    heads = wo_ref.shape[1] // att_ref.shape[2]
    attended = jnp.concatenate([att_ref[:, j, :] for j in range(heads)], axis=1).astype(jnp.bfloat16)

    def project(c, carry):
        span = pl.ds(pl.multiple_of(c * cols, cols), cols)
        weights = jnp.concatenate([wo_ref[c * strips + i] for i in range(strips)], axis=1)
        out = jnp.dot(attended, weights, preferred_element_type=jnp.float32)
        y_ref[:, span] = (x_ref[:, span].astype(jnp.float32) + out).astype(jnp.bfloat16)
        return carry

    lax.fori_loop(0, y_ref.shape[1] // cols, project, 0)
    y_copy = pltpu.make_async_copy(y_ref, y_out, y_sem)
    y_copy.start()
    for copy in copies:
        copy.wait()
    y_copy.wait()


def solution(mesh):
    n = mesh.shape['cp']
    batch_spec = P(('dp', 'cp'))
    seq_spec = P('dp', 'cp')
    whole = P()
    hbm = pl.BlockSpec(memory_space=pl.ANY)
    vmem = pl.BlockSpec(memory_space=pltpu.VMEM)

    def per_device(x_tok, prompt_lens, k_cache, v_cache, norm_gain, w_q, b_q, w_k, b_k, w_v, b_v, w_o):
        rows, d_model = x_tok.shape
        batch, slots, kv_heads, head = k_cache.shape
        q_cols = w_q.shape[1]
        heads = q_cols // head
        q_rows = -(-heads // PACK) * PACK
        tiles = slots * kv_heads // PACK
        all_tiles = tiles * n
        block_rows = tiles * PACK
        cols = w_k.shape[1]
        half = head // 2
        freq = np.power(ROPE_THETA, -np.arange(half) * 2.0 / head).astype(np.float32)
        freq = jnp.asarray(np.concatenate([freq, freq])[None])
        parts = 4

        bf16, f32 = jnp.bfloat16, jnp.float32
        kbuf, vbuf, wo, att, x_near = pl.pallas_call(
            functools.partial(gather_kernel, n, kv_heads),
            out_shape=[
                pltpu.VMEM((rows, all_tiles, PACK, head), bf16),
                pltpu.VMEM((rows, all_tiles, PACK, head), bf16),
                pltpu.VMEM((w_o.shape[1] // LANES, w_o.shape[0], LANES), bf16),
                pltpu.VMEM((rows, q_rows, head), f32),
                pltpu.VMEM((rows, d_model), bf16),
            ],
            in_specs=[hbm] * 13,
            out_specs=[vmem] * 5,
            scratch_shapes=[
                pltpu.SMEM((batch,), jnp.int32),
                pltpu.VMEM((1, head), f32),
                pltpu.VMEM((d_model,), bf16),
                pltpu.VMEM((q_cols,), bf16),
                pltpu.VMEM((cols,), bf16),
                pltpu.VMEM((cols,), bf16),
                pltpu.VMEM((3, d_model, cols), bf16),
                pltpu.VMEM((rows, d_model), bf16),
                pltpu.VMEM((rows, q_rows, head), f32),
                pltpu.VMEM((rows, PACK, head), f32),
                pltpu.VMEM((rows, PACK, head), f32),
                pltpu.VMEM((rows, n, q_rows, block_rows), f32),
                pltpu.VMEM((rows, n, q_rows, block_rows), bf16),
                pltpu.VMEM((rows, q_rows, head), f32),
                pltpu.VMEM((rows, q_rows, head), f32),
                pltpu.SemaphoreType.DMA((7,)),
                pltpu.SemaphoreType.DMA((3,)),
                pltpu.SemaphoreType.DMA((w_o.shape[1] // LANES,)),
                pltpu.SemaphoreType.DMA((n,)),
                pltpu.SemaphoreType.DMA((n,)),
                pltpu.SemaphoreType.DMA((n, parts)),
                pltpu.SemaphoreType.DMA((n, parts)),
                pltpu.SemaphoreType.REGULAR,
            ],
            compiler_params=pltpu.CompilerParams(collective_id=0, has_side_effects=True, vmem_limit_bytes=28 * 1024 * 1024),
            name='gather_attend',
        )(prompt_lens, x_tok, freq, norm_gain, w_q, b_q, w_k, b_k, w_v, b_v, w_o,
          k_cache.reshape(batch, tiles, PACK, head), v_cache.reshape(batch, tiles, PACK, head))

        y_out, k_out, v_out = pl.pallas_call(
            finish_kernel,
            out_shape=[
                jax.ShapeDtypeStruct(x_tok.shape, bf16),
                jax.ShapeDtypeStruct(kbuf.shape, bf16),
                jax.ShapeDtypeStruct(vbuf.shape, bf16),
            ],
            in_specs=[vmem] * 5,
            out_specs=[hbm] * 3,
            scratch_shapes=[pltpu.VMEM(x_tok.shape, bf16), pltpu.SemaphoreType.DMA((2, rows)), pltpu.SemaphoreType.DMA],
            compiler_params=pltpu.CompilerParams(vmem_limit_bytes=28 * 1024 * 1024),
            name='finish',
        )(*[pltpu.with_memory_space_constraint(a, pltpu.VMEM) for a in (kbuf, vbuf, wo, att, x_near)])
        shape = (rows, slots * n, kv_heads, head)
        return y_out, k_out.reshape(shape), v_out.reshape(shape)

    return jax.shard_map(per_device, mesh=mesh, in_specs=(batch_spec, P('dp'), seq_spec, seq_spec, whole, whole, whole, whole, whole, whole, whole, whole), out_specs=(batch_spec, batch_spec, batch_spec), check_vma=False)
```
